32 devices in a mesh: dp: 2 (over x), ep: 16 (over z, y, core).
Axes of the slice: x: 2, y: 2, z: 4, core: 2. Of those that a mesh axis runs over, the one named last changes fastest.
Arguments:
- x_tokens: bfloat16 [4096, 1536], P(('dp', 'ep')), parts along dimension 0
- slot_expert: int32 [320], replicated
- w1_slots: bfloat16 [320, 1536, 512], P('ep')
- w3_slots: bfloat16 [320, 1536, 512], P('ep')
- w2_slots: bfloat16 [320, 512, 1536], P('ep')
- assign: int32 [4096, 6], P(('dp', 'ep')), parts along dimension 0
- w_router: bfloat16 [1536, 64], replicated
- w1_shared: bfloat16 [1536, 1024], replicated
- w3_shared: bfloat16 [1536, 1024], replicated
- w2_shared: bfloat16 [1024, 1536], replicated
Outputs:
- output: bfloat16 [4096, 1536], P(('dp', 'ep')), parts along dimension 0
There are 2 independent parts. The reference program is written for one: setup_inputs(seed, part) draws one part's arguments, and reference() takes and returns one part's arrays. A program takes and returns all parts, laid end to end along the dimension named above; an argument that names none is the same for every part.
All inputs are finite; a program needn't handle non-finite values.
Results may differ from the reference program's by a relative error of at most 0.001.
Values are sent between devices in bfloat16 or wider.
A program may use at most 1 GiB of HBM per device.

```python
import jax
import jax.numpy as jnp
from jax import lax

DIM_MODEL = 1536
FF_EXPERT = 512
FF_SHARED = 1024
NUM_EXPERTS = 64
TOP_K = 6
NUM_SLOTS = 320
GROUP_SIZE = 16
TOK_DEV = 128

TOKENS = TOK_DEV * GROUP_SIZE
CAP_ROWS = max(4, (3 * TOK_DEV * TOP_K) // NUM_SLOTS)
SEG_ROWS = min(TOKENS, GROUP_SIZE * CAP_ROWS)
ROUTE_SCALE = 2.5


def draw_routing(key_shared, key_part):
    key_rank, key_place = jax.random.split(key_shared, 2)
    rank_expert = jax.random.permutation(key_rank, NUM_EXPERTS).astype(jnp.int32)
    base_of_slot = jax.random.permutation(key_place, NUM_SLOTS).astype(jnp.int32)
    slot_expert = rank_expert[base_of_slot % NUM_EXPERTS]
    slot_of_base = jnp.argsort(base_of_slot).astype(jnp.int32)
    key_noise, key_coin, key_pick = jax.random.split(key_part, 3)
    rank_ids = jnp.arange(NUM_EXPERTS, dtype=jnp.int32)
    rank_bias = (2 * TOP_K * 4096) // (NUM_EXPERTS * (rank_ids + 1))
    noise_int = jax.random.randint(key_noise, (TOKENS, NUM_EXPERTS), 0, 4096, dtype=jnp.int32)
    token_ids = jnp.arange(TOKENS, dtype=jnp.int32)
    forced = token_ids < CAP_ROWS
    force_bonus = jnp.where(forced[:, None] & (rank_ids[None, :] == 0), 16384, 0)
    rank_score = (noise_int + rank_bias[None, :] + force_bonus) * NUM_EXPERTS + rank_ids[None, :]
    chosen_rank = lax.top_k(rank_score, TOP_K)[1].astype(jnp.int32)
    copies = (NUM_SLOTS - 1 - chosen_rank) // NUM_EXPERTS + 1
    coin_flip = jax.random.randint(key_coin, (TOKENS, TOP_K), 0, 2, dtype=jnp.int32)
    pick_copy = jax.random.randint(key_pick, (TOKENS, TOP_K), 0, 65536, dtype=jnp.int32) % copies
    keep_first = (coin_flip == 0) | (forced[:, None] & (chosen_rank == 0))
    copy_index = jnp.where(keep_first, 0, pick_copy)
    slot_pick = slot_of_base[chosen_rank + copy_index * NUM_EXPERTS]
    device_of = (token_ids // TOK_DEV)[:, None]
    group_key = (device_of * NUM_SLOTS + slot_pick).reshape(-1)
    sort_order = jnp.argsort(group_key, stable=True)
    sorted_key = group_key[sort_order]
    first_pos = jnp.searchsorted(sorted_key, sorted_key, side='left').astype(jnp.int32)
    rank_sorted = jnp.arange(TOKENS * TOP_K, dtype=jnp.int32) - first_pos
    rank_flat = jnp.zeros((TOKENS * TOP_K,), jnp.int32).at[sort_order].set(rank_sorted)
    assign = jnp.where(rank_flat < CAP_ROWS, slot_pick.reshape(-1), -1).reshape(TOKENS, TOP_K)
    return slot_expert, assign.astype(jnp.int32)


def setup_inputs(seed: int = 0, part: int = 0) -> dict:
    weight_keys = jax.random.split(jax.random.key(seed), 8)
    part_key = jax.random.fold_in(jax.random.key(seed + 1), part)
    key_tokens, key_route = jax.random.split(part_key, 2)
    slot_expert, assign = draw_routing(weight_keys[0], key_route)
    x_tokens = jax.random.normal(key_tokens, (TOKENS, DIM_MODEL), jnp.float32)
    w1_experts = jax.random.normal(weight_keys[1], (NUM_EXPERTS, DIM_MODEL, FF_EXPERT), jnp.float32) * DIM_MODEL ** -0.5
    w3_experts = jax.random.normal(weight_keys[2], (NUM_EXPERTS, DIM_MODEL, FF_EXPERT), jnp.float32) * DIM_MODEL ** -0.5
    w2_experts = jax.random.normal(weight_keys[3], (NUM_EXPERTS, FF_EXPERT, DIM_MODEL), jnp.float32) * FF_EXPERT ** -0.5
    w_router = jax.random.normal(weight_keys[4], (DIM_MODEL, NUM_EXPERTS), jnp.float32) * DIM_MODEL ** -0.5
    w1_shared = jax.random.normal(weight_keys[5], (DIM_MODEL, FF_SHARED), jnp.float32) * DIM_MODEL ** -0.5
    w3_shared = jax.random.normal(weight_keys[6], (DIM_MODEL, FF_SHARED), jnp.float32) * DIM_MODEL ** -0.5
    w2_shared = jax.random.normal(weight_keys[7], (FF_SHARED, DIM_MODEL), jnp.float32) * FF_SHARED ** -0.5
    return {
        'x_tokens': x_tokens.astype(jnp.bfloat16),
        'slot_expert': slot_expert,
        'w1_slots': w1_experts.astype(jnp.bfloat16)[slot_expert],
        'w3_slots': w3_experts.astype(jnp.bfloat16)[slot_expert],
        'w2_slots': w2_experts.astype(jnp.bfloat16)[slot_expert],
        'assign': assign,
        'w_router': w_router.astype(jnp.bfloat16),
        'w1_shared': w1_shared.astype(jnp.bfloat16),
        'w3_shared': w3_shared.astype(jnp.bfloat16),
        'w2_shared': w2_shared.astype(jnp.bfloat16),
    }


def gate_weights(x_tokens, assign, slot_expert, w_router):
    logits = jnp.dot(x_tokens, w_router, preferred_element_type=jnp.float32)
    gate_prob = jax.nn.sigmoid(logits)
    is_kept = assign >= 0
    chosen = slot_expert[jnp.maximum(assign, 0)]
    picked = jnp.where(is_kept, jnp.take_along_axis(gate_prob, chosen, axis=1), 0.0)
    gate_total = jnp.sum(picked, axis=1, keepdims=True)
    return ROUTE_SCALE * picked / jnp.maximum(gate_total, 1e-30), is_kept


def shared_expert(x_tokens, w1_shared, w3_shared, w2_shared):
    h_gate = jnp.dot(x_tokens, w1_shared, preferred_element_type=jnp.float32)
    h_up = jnp.dot(x_tokens, w3_shared, preferred_element_type=jnp.float32)
    mid_act = (jax.nn.silu(h_gate) * h_up).astype(jnp.bfloat16)
    return jnp.dot(mid_act, w2_shared, preferred_element_type=jnp.float32)


def reference(x_tokens, slot_expert, w1_slots, w3_slots, w2_slots, assign, w_router, w1_shared, w3_shared, w2_shared):
    route_weight, is_kept = gate_weights(x_tokens, assign, slot_expert, w_router)
    shared_out = shared_expert(x_tokens, w1_shared, w3_shared, w2_shared)
    flat_slot = jnp.where(is_kept, assign, NUM_SLOTS).reshape(-1)
    sort_order = jnp.argsort(flat_slot, stable=True)
    sorted_slot = flat_slot[sort_order]
    slot_ids = jnp.arange(NUM_SLOTS, dtype=jnp.int32)
    seg_start = jnp.searchsorted(sorted_slot, slot_ids, side='left').astype(jnp.int32)
    seg_end = jnp.searchsorted(sorted_slot, slot_ids, side='right').astype(jnp.int32)
    token_list = jnp.concatenate([(sort_order // TOP_K).astype(jnp.int32), jnp.zeros((SEG_ROWS,), jnp.int32)])
    weight_list = jnp.concatenate([route_weight.reshape(-1)[sort_order], jnp.zeros((SEG_ROWS,), route_weight.dtype)])
    row_offsets = jnp.arange(SEG_ROWS, dtype=jnp.int32)

    def slot_step(acc_rows, slot_id):
        seg_begin = seg_start[slot_id]
        row_ids = lax.dynamic_slice(token_list, (seg_begin,), (SEG_ROWS,))
        row_weight = lax.dynamic_slice(weight_list, (seg_begin,), (SEG_ROWS,))
        row_weight = jnp.where(row_offsets < seg_end[slot_id] - seg_begin, row_weight, 0.0)
        x_rows = x_tokens[row_ids]
        h_gate = jnp.dot(x_rows, w1_slots[slot_id], preferred_element_type=jnp.float32)
        h_up = jnp.dot(x_rows, w3_slots[slot_id], preferred_element_type=jnp.float32)
        mid_act = (jax.nn.silu(h_gate) * h_up).astype(jnp.bfloat16)
        out_rows = jnp.dot(mid_act, w2_slots[slot_id], preferred_element_type=jnp.float32).astype(jnp.bfloat16)
        acc_rows = acc_rows.at[row_ids].add(row_weight[:, None] * out_rows.astype(jnp.float32))
        return acc_rows, None

    routed = lax.scan(slot_step, jnp.zeros((TOKENS, DIM_MODEL), jnp.float32), slot_ids)[0]
    return (shared_out + routed).astype(jnp.bfloat16)
```

```python
import functools

import jax
import jax.numpy as jnp
from jax import lax
from jax.experimental import pallas as pl
from jax.experimental.pallas import tpu as pltpu
from jax.sharding import PartitionSpec as P

ROUTE_SCALE = 2.5
MESH = pl.DeviceIdType.MESH
NUM_EXPERTS = 64
EXT = 64
UNIT = 128
NBUF = 6
F32, BF16, I32 = jnp.float32, jnp.bfloat16, jnp.int32


def dims():
    me = lax.axis_index("ep")
    c, y, z, h = me % 2, (me // 2) % 2, (me // 4) % 2, me // 8
    sib = me + 1 - 2 * c
    yn = me + 2 - 4 * y
    zn = me + 4 - 8 * z
    mir = me + 8 - 16 * h
    first = yn + c * (zn - yn)
    second = zn + c * (yn - zn)
    diag = yn + zn - me
    return me, c, h, sib, yn, zn, mir, first, second, diag


def barrier(peers):
    sem = pltpu.get_barrier_semaphore()
    for peer in peers:
        pl.semaphore_signal(sem, inc=1, device_id=peer, device_id_type=MESH)
    pl.semaphore_wait(sem, len(peers))


def dot(a, b, ca=1, cb=0):
    return lax.dot_general(a, b, (((ca,), (cb,)), ((), ())), preferred_element_type=F32)


def split3(v):
    hi = v.astype(BF16)
    rest = v - hi.astype(F32)
    mid = rest.astype(BF16)
    lo = (rest - mid.astype(F32)).astype(BF16)
    return hi, mid, lo


def gather_kernel(x_ref, at_ref, se_ref, wr_ref, rnd_ref, w1_hbm, w3_hbm, w2_hbm,
                  xm_out, xe_out, wm_out, we_out, own_out, gw_out, z_out, nr_out,
                  xs, xes, wms, wes, xcr, wcr, xsnd, wsnd, cand_s, own_s, flag_s, frecv,
                  w1s, w3s, w2s, ssem, rsem, lsem):
    me, c, h, sib, yn, zn, mir, first, second, diag = dims()
    dp = lax.axis_index("dp")
    qm, qf, qs, qg = me % 8, first % 8, second % 8, diag % 8
    loads = [pltpu.make_async_copy(a, b, lsem.at[i]) for i, (a, b) in
             enumerate(((w1_hbm, w1s), (w3_hbm, w3s), (w2_hbm, w2s)))]
    for cp in loads:
        cp.start()
    barrier([{"ep": sib}, {"ep": yn}, {"ep": zn}, {"ep": mir}, {"dp": 1 - dp}])

    def rcopy(src, dst, i, dev):
        return pltpu.make_async_remote_copy(src_ref=src, dst_ref=dst, send_sem=ssem.at[i], recv_sem=rsem.at[i],
                                            device_id=dev, device_id_type=MESH)

    def spread(own, buf, base):
        ep = lambda d: {"ep": d}
        return [rcopy(own, buf.at[qm], base, ep(first)), rcopy(own, buf.at[qm], base + 1, ep(second)),
                rcopy(own, buf.at[qm], base + 2, ep(sib)), rcopy(buf.at[qf], buf.at[qf], base + 3, ep(second)),
                rcopy(buf.at[qf], buf.at[qf], base + 4, ep(sib)), rcopy(buf.at[qs], buf.at[qs], base + 5, ep(sib)),
                rcopy(buf.at[qg], buf.at[qg], base + 6, ep(sib))]

    ax = spread(x_ref, xs, 0)
    for i in range(3):
        ax[i].start()

    n_slots = se_ref.shape[1]
    n_tok = x_ref.shape[0]
    rnd = rnd_ref[0:1, 0:1]
    first_round = jnp.where(rnd == 0.0, 1.0, 0.0)
    logits = lax.dot_general(wr_ref[...], x_ref[...], (((0,), (1,)), ((), ())), preferred_element_type=F32)
    gate = jax.nn.sigmoid(logits)
    expert_of = se_ref[...]
    eye = (lax.broadcasted_iota(I32, (NUM_EXPERTS, n_slots), 0) == expert_of).astype(F32)
    eye_bf = eye.astype(BF16)
    lane_slot = lax.broadcasted_iota(I32, (1, n_slots), 1)
    per_half = n_slots // 2
    here = jnp.where((lane_slot >= h * per_half) & (lane_slot < (h + 1) * per_half), 1.0, 0.0)
    avail = jnp.where(jnp.sum(eye * here, axis=1, keepdims=True) > 0.0, 1.0, 0.0)
    row_slot = lax.broadcasted_iota(I32, (n_slots, n_tok), 0)
    picks = []
    for k in range(6):
        hot = (row_slot == at_ref[k:k + 1, :]).astype(F32).astype(BF16)
        picks.append(dot(eye_bf, hot))
    chosen = functools.reduce(lambda a, b: a + b, picks)
    picked = gate * chosen
    total = jnp.sum(picked, axis=0, keepdims=True)
    weight = ROUTE_SCALE * picked / jnp.maximum(total, 1e-30)
    xs[qm] = x_ref[...]
    wm_own = weight * (avail * first_round)
    wsnd[0] = wm_own
    wms[qm] = wm_own
    aw = spread(wsnd.at[0], wms, 7)
    for i in range(3):
        aw[i].start()

    miss = [jnp.sum(p * (1.0 - avail), axis=0, keepdims=True) for p in picks]
    miss_all = jnp.concatenate(miss + [jnp.zeros((2, n_tok), F32)], axis=0)
    upper = (lax.broadcasted_iota(I32, (n_tok, n_tok), 0) < lax.broadcasted_iota(I32, (n_tok, n_tok), 1))
    before = dot(miss_all.astype(BF16), upper.astype(F32).astype(BF16))
    offset = -EXT * rnd
    count = jnp.zeros((1, 1), F32)
    row_ext = lax.broadcasted_iota(I32, (EXT, n_tok), 0).astype(F32)
    take = jnp.zeros((EXT, n_tok), F32)
    expert_hot = jnp.zeros((NUM_EXPERTS, EXT), F32)
    home = jnp.zeros((EXT, n_tok), F32)
    for k in range(6):
        sel = jnp.where((row_ext == before[k:k + 1, :] + offset) & (miss[k] > 0.0), 1.0, 0.0)
        take += sel
        expert_hot += dot(picks[k].astype(BF16), sel.astype(BF16), 1, 1)
        home += sel * jnp.sum(picks[k] * weight, axis=0, keepdims=True)
        mk = jnp.sum(miss[k], axis=1, keepdims=True)
        offset += mk
        count += mk
    gw_out[...] = home
    xsnd[...] = dot(take.astype(BF16), x_ref[...]).astype(BF16)
    wsnd[1] = jnp.concatenate([expert_hot, jnp.zeros((NUM_EXPERTS, 128 - EXT), F32)], axis=1)
    cross = [rcopy(xsnd, xcr, 28, {"ep": mir}), rcopy(wsnd.at[1], wcr, 29, {"ep": mir})]
    for cp in cross:
        cp.start()
    flag_s[0] = jnp.broadcast_to(jnp.floor((count + (EXT - 1)) * (1.0 / EXT)), (8, 128))
    steps = [rcopy(flag_s.at[i], frecv.at[i], 30 + i, d) for i, d in
             enumerate(({"dp": 1 - dp}, {"ep": sib}, {"ep": mir}, {"ep": zn}, {"ep": yn}))]
    steps[0].start()

    slot_row = lax.broadcasted_iota(I32, (n_slots, 128), 0)
    lane_dev = lax.broadcasted_iota(I32, (n_slots, 128), 1)
    lo = (lane_dev + 8 * h) * (n_slots // 16)
    block = ((slot_row >= lo) & (slot_row < lo + n_slots // 16) & (lane_dev < 8)).astype(F32).astype(BF16)
    cand = jnp.where(dot(eye_bf, block) > 0.0, 1.0, 0.0)
    n_cand = jnp.sum(cand, axis=1, keepdims=True)
    cand_s[...] = cand
    load0 = jnp.sum(cand * jnp.where(n_cand == 1.0, 1.0, 0.0), axis=0, keepdims=True)
    lane = lax.broadcasted_iota(I32, (1, 128), 1).astype(F32)

    def pick(e, load):
        row = cand_s[pl.ds(e, 1), :]
        key = jnp.where(row > 0.0, load * 256.0 + lane, 1e9)
        best = jnp.min(key, axis=1, keepdims=True)
        sel = jnp.where((key == best) & (row > 0.0), 1.0, 0.0)
        own_s[pl.ds(e, 1), :] = sel
        several = jnp.where(jnp.sum(row, axis=1, keepdims=True) > 1.0, 1.0, 0.0)
        return load + sel * several

    lax.fori_loop(0, NUM_EXPERTS, pick, load0)
    mine = jnp.where(lax.broadcasted_iota(I32, (8, 128), 1) == qm, 1.0, 0.0)
    own = dot(mine.astype(BF16), own_s[...].astype(BF16), 1, 1)
    own_out[...] = jnp.concatenate([own, jnp.zeros((8, 128 - NUM_EXPERTS), F32)], axis=1).astype(I32)

    for i in range(4):
        steps[i].wait()
        flag_s[i + 1] = jnp.maximum(flag_s[i], frecv[i])
        steps[i + 1].start()

    for a in (ax, aw):
        a[0].wait_recv()
        a[3].start()
        a[4].start()
    for a in (ax, aw):
        a[1].wait_recv()
        a[5].start()
    for cp in cross:
        cp.wait()
    xes[qm] = xcr[...]
    wes[qm] = wcr[...]
    ex = spread(xcr, xes, 14)
    ew = spread(wcr, wes, 21)
    for a in (ex, ew):
        for i in range(3):
            a[i].start()
    steps[4].wait()
    nr_out[...] = jnp.maximum(flag_s[4], frecv[4])

    for cp in loads:
        cp.wait()
    hg = dot(x_ref[...], w1s[...])
    hu = dot(x_ref[...], w3s[...])
    act = (jax.nn.silu(hg) * hu).astype(BF16)
    z_out[...] = dot(act, w2s[...]) * first_round

    for a in (ax, aw):
        a[3].wait_recv()
        a[6].start()
    for a in (ex, ew):
        a[0].wait_recv()
        a[3].start()
        a[4].start()
    for a in (ex, ew):
        a[1].wait_recv()
        a[5].start()
    for a in (ax, aw):
        for i in (2, 4, 5, 6):
            a[i].wait_recv()
    outs = [pltpu.make_async_copy(xs, xm_out, lsem.at[3]), pltpu.make_async_copy(wms, wm_out, lsem.at[4])]
    for cp in outs:
        cp.start()
    for a in (ex, ew):
        a[3].wait_recv()
        a[6].start()
    for a in (ex, ew):
        for i in (2, 4, 5, 6):
            a[i].wait_recv()
    outs += [pltpu.make_async_copy(xes, xe_out, lsem.at[5]), pltpu.make_async_copy(wes, we_out, lsem.at[6])]
    for cp in outs[2:]:
        cp.start()
    for a in (ax, aw, ex, ew):
        for cp in a:
            cp.wait_send()
    for cp in outs:
        cp.wait()


def expert_kernel(own_ref, se_ref, xm_hbm, xe_hbm, wm_ref, we_ref, w1_hbm, w3_hbm, w2_hbm, pm_out, pe_out,
                  xv, wrow, rank, pv, gt, ocat, b1, b3, b2, slots, experts, seen, wsem, xsem):
    me = lax.axis_index("ep")
    n_local = w1_hbm.shape[0]
    n_main, n_ext = 8 * 128, 8 * EXT
    n_tok = n_main + n_ext
    xl = [pltpu.make_async_copy(xm_hbm, xv.at[pl.ds(0, n_main)], xsem.at[0]),
          pltpu.make_async_copy(xe_hbm, xv.at[pl.ds(n_main, n_ext)], xsem.at[1])]
    for cp in xl:
        cp.start()

    def clear(e, carry):
        seen[e] = 0
        return carry

    lax.fori_loop(0, NUM_EXPERTS, clear, 0)

    def listing(s, n):
        e = se_ref[me * n_local + s]
        use = (own_ref[0, e] == 1) & (seen[e] == 0)

        @pl.when(use)
        def _():
            slots[n] = s
            experts[n] = e
            seen[e] = 1
        return jnp.where(use, n + 1, n)

    n_act = lax.fori_loop(0, n_local, listing, 0)

    def fetch(i):
        s, b = slots[i], lax.rem(i, NBUF)
        return [pltpu.make_async_copy(w1_hbm.at[s], b1.at[b], wsem.at[0, b]),
                pltpu.make_async_copy(w3_hbm.at[s], b3.at[b], wsem.at[1, b]),
                pltpu.make_async_copy(w2_hbm.at[s], b2.at[b], wsem.at[2, b])]

    def start(i):
        @pl.when(i < n_act)
        def _():
            for cp in fetch(i):
                cp.start()

    for i in range(NBUF):
        start(i)

    upper = (lax.broadcasted_iota(I32, (128, 128), 0) < lax.broadcasted_iota(I32, (128, 128), 1))
    upper = upper.astype(F32).astype(BF16)
    run = jnp.zeros((NUM_EXPERTS, 1), F32)
    for j in range(n_tok // 128):
        if j < 8:
            w = wm_ref[j]
        else:
            w = jnp.concatenate([we_ref[2 * (j - 8)][:, :EXT], we_ref[2 * (j - 8) + 1][:, :EXT]], axis=1)
        mask = jnp.where(w != 0.0, 1.0, 0.0)
        pos = dot(mask.astype(BF16), upper) + run
        run += jnp.sum(mask, axis=1, keepdims=True)
        rank[:, j * 128:(j + 1) * 128] = jnp.where(mask > 0.0, pos, -1.0)
        wrow[:, j * 128:(j + 1) * 128] = w
    pv[...] = jnp.zeros_like(pv)
    for cp in xl:
        cp.wait()

    def one(i, carry):
        for cp in fetch(i):
            cp.wait()
        e, b = experts[i], lax.rem(i, NBUF)
        pos = rank[pl.ds(e, 1), :]
        units = (jnp.max(pos).astype(I32) + UNIT) // UNIT

        def unit(u, carry):
            rows = lax.broadcasted_iota(I32, (UNIT, n_tok), 0) + u * UNIT
            hit = rows.astype(F32) == rank[pl.ds(e, 1), :]
            g = jnp.where(hit, 1.0, 0.0)
            wcol = jnp.sum(jnp.where(hit, wrow[pl.ds(e, 1), :], 0.0), axis=1, keepdims=True)
            xg = dot(g.astype(BF16), xv[...]).astype(BF16)
            act = (jax.nn.silu(dot(xg, b1[b])) * dot(xg, b3[b])).astype(BF16)
            o = dot(act, b2[b]).astype(BF16)
            for j, part in enumerate(split3(wcol * o.astype(F32))):
                ocat[j * UNIT:(j + 1) * UNIT, :] = part
            gt[...] = jnp.transpose(g).astype(BF16)

            def rows_of(m, carry):
                rs = pl.ds(pl.multiple_of(m * 256, 256), 256)
                left = gt[rs, :]
                pv[rs, :] += dot(jnp.concatenate([left, left, left], axis=1), ocat[...])
                return carry
            return lax.fori_loop(0, n_tok // 256, rows_of, carry)

        lax.fori_loop(0, units, unit, 0)
        start(i + NBUF)
        return carry

    lax.fori_loop(0, n_act, one, 0)
    outs = [pltpu.make_async_copy(pv.at[pl.ds(0, n_main)], pm_out, xsem.at[0]),
            pltpu.make_async_copy(pv.at[pl.ds(n_main, n_ext)], pe_out, xsem.at[1])]
    for cp in outs:
        cp.start()
    for cp in outs:
        cp.wait()


def scatter_kernel(pm_hbm, pe_hbm, acc_ref, z_ref, gw_ref, out_ref,
                   mo, md, mrg, mrf, mrs, mfin, eo, ed, erg, erf, ers, efin, esnd, ecr, ssem, rsem, lsem):
    me, c, h, sib, yn, zn, mir, first, second, diag = dims()
    cols = mo.shape[-1]
    mine = pl.ds(pl.multiple_of(c * cols, 128), cols)
    theirs = pl.ds(pl.multiple_of((1 - c) * cols, 128), cols)
    chips = [(d % 8) // 2 for d in (diag, first, second, me)]
    local, peer = [], []
    for base, (src, own, got) in ((0, (pe_hbm, eo, ed)), (4, (pm_hbm, mo, md))):
        for i, chip in enumerate(chips):
            rows = pl.ds(2 * chip, 2)
            sib_rows = pl.ds(2 * chips[(0, 2, 1, 3)[i]], 2)
            local.append(pltpu.make_async_copy(src.at[rows, :, mine], own.at[i], lsem.at[base + i]))
            peer.append(pltpu.make_async_remote_copy(
                src_ref=src.at[sib_rows, :, theirs], dst_ref=got.at[i], send_sem=ssem.at[base + i],
                recv_sem=rsem.at[base + i], device_id={"ep": sib}, device_id_type=MESH))
    for cp in local:
        cp.start()
    barrier([{"ep": sib}, {"ep": yn}, {"ep": zn}, {"ep": mir}])
    for cp in peer:
        cp.start()

    def rcopy(src, dst, i, dev):
        return pltpu.make_async_remote_copy(src_ref=src, dst_ref=dst, send_sem=ssem.at[i], recv_sem=rsem.at[i],
                                            device_id={"ep": dev}, device_id_type=MESH)

    def sends(own, rg, rf, rs, fin, base):
        return [rcopy(own.at[0], rg, base, first), rcopy(own.at[1], rf, base + 1, first),
                rcopy(own.at[2], rs, base + 2, second), rcopy(own.at[3, 1 - c], fin, base + 3, sib)]

    se = sends(eo, erg, erf, ers, efin, 8)
    sm = sends(mo, mrg, mrf, mrs, mfin, 12)
    back = rcopy(esnd, ecr, 16, mir)

    def joined(own, got, i, base):
        local[base + i].wait()
        peer[base + i].wait_recv()
        own[i] = own[i] + got[i]

    joined(eo, ed, 0, 0)
    se[0].start()
    joined(mo, md, 0, 4)
    sm[0].start()
    joined(eo, ed, 1, 0)
    se[1].start()
    joined(mo, md, 1, 4)
    sm[1].start()
    joined(eo, ed, 2, 0)
    joined(eo, ed, 3, 0)
    joined(mo, md, 2, 4)
    joined(mo, md, 3, 4)
    se[0].wait_recv()
    eo[2] = eo[2] + erg[...]
    se[2].start()
    sm[0].wait_recv()
    mo[2] = mo[2] + mrg[...]
    sm[2].start()
    se[1].wait_recv()
    se[2].wait_recv()
    eo[3] = eo[3] + erf[...] + ers[...]
    se[3].start()
    se[3].wait_recv()
    esnd[:, mine] = eo[3, c].astype(BF16)
    esnd[:, theirs] = efin[...].astype(BF16)
    back.start()
    sm[1].wait_recv()
    mo[3] = mo[3] + mrf[...]
    back.wait_recv()
    out_ref[...] = acc_ref[...] + z_ref[...]
    for part in split3(gw_ref[...]):
        out_ref[...] += dot(part, ecr[...], 0, 0)
    sm[2].wait_recv()
    mo[3] = mo[3] + mrs[...]
    sm[3].start()
    out_ref[:, mine] += mo[3, c]
    sm[3].wait_recv()
    out_ref[:, theirs] += mfin[...]
    for cp in peer + se + sm + [back]:
        cp.wait_send()


def solution(mesh):
    any_space = pl.BlockSpec(memory_space=pl.ANY)
    vmem = pl.BlockSpec(memory_space=pltpu.VMEM)
    smem = pl.BlockSpec(memory_space=pltpu.SMEM)
    sds = jax.ShapeDtypeStruct

    def gather(x, at, se, wr, rnd, w1, w3, w2):
        d, ff = w1.shape
        return pl.pallas_call(
            gather_kernel,
            out_shape=(sds((8, 128, d), BF16), sds((8, EXT, d), BF16), sds((8, NUM_EXPERTS, 128), F32),
                       sds((8, NUM_EXPERTS, 128), F32), sds((8, 128), I32), sds((EXT, 128), F32),
                       sds((128, d), F32), sds((8, 128), F32)),
            in_specs=[vmem] * 5 + [any_space] * 3,
            out_specs=(any_space,) * 4 + (vmem,) * 4,
            scratch_shapes=[
                pltpu.VMEM((8, 128, d), BF16), pltpu.VMEM((8, EXT, d), BF16),
                pltpu.VMEM((8, NUM_EXPERTS, 128), F32), pltpu.VMEM((8, NUM_EXPERTS, 128), F32),
                pltpu.VMEM((EXT, d), BF16), pltpu.VMEM((NUM_EXPERTS, 128), F32),
                pltpu.VMEM((EXT, d), BF16), pltpu.VMEM((2, NUM_EXPERTS, 128), F32),
                pltpu.VMEM((NUM_EXPERTS, 128), F32), pltpu.VMEM((NUM_EXPERTS, 128), F32),
                pltpu.VMEM((5, 8, 128), F32), pltpu.VMEM((5, 8, 128), F32),
                pltpu.VMEM((d, ff), BF16), pltpu.VMEM((d, ff), BF16), pltpu.VMEM((ff, d), BF16),
                pltpu.SemaphoreType.DMA((35,)), pltpu.SemaphoreType.DMA((35,)), pltpu.SemaphoreType.DMA((7,)),
            ],
            compiler_params=pltpu.CompilerParams(collective_id=0, has_side_effects=True),
            name="gather_rows",
        )(x, at, se, wr, rnd, w1, w3, w2)

    def experts(own, se, xm, xe, wm, we, w1, w3, w2):
        _, d, ff = w1.shape
        n_tok = 8 * (128 + EXT)
        return pl.pallas_call(
            expert_kernel,
            out_shape=(sds((8 * 128, d), F32), sds((8 * EXT, d), F32)),
            in_specs=[smem, smem, any_space, any_space, vmem, vmem] + [any_space] * 3,
            out_specs=(any_space, any_space),
            scratch_shapes=[
                pltpu.VMEM((n_tok, d), BF16), pltpu.VMEM((NUM_EXPERTS, n_tok), F32), pltpu.VMEM((NUM_EXPERTS, n_tok), F32),
                pltpu.VMEM((n_tok, d), F32), pltpu.VMEM((n_tok, UNIT), BF16), pltpu.VMEM((3 * UNIT, d), BF16),
                pltpu.VMEM((NBUF, d, ff), BF16), pltpu.VMEM((NBUF, d, ff), BF16), pltpu.VMEM((NBUF, ff, d), BF16),
                pltpu.SMEM((32,), I32), pltpu.SMEM((32,), I32), pltpu.SMEM((NUM_EXPERTS,), I32),
                pltpu.SemaphoreType.DMA((3, NBUF)), pltpu.SemaphoreType.DMA((2,)),
            ],
            name="expert_rows",
        )(own, se, xm, xe, wm, we, w1, w3, w2)

    def scatter(pm, pe, acc, z, gw):
        d = acc.shape[1]
        half = d // 2
        big, small = (2, 128, half), (2, EXT, half)
        return pl.pallas_call(
            scatter_kernel,
            out_shape=sds((128, d), F32),
            in_specs=[any_space, any_space, vmem, vmem, vmem],
            out_specs=vmem,
            scratch_shapes=[
                pltpu.VMEM((4,) + big, F32), pltpu.VMEM((4,) + big, F32),
                pltpu.VMEM(big, F32), pltpu.VMEM(big, F32), pltpu.VMEM(big, F32), pltpu.VMEM((128, half), F32),
                pltpu.VMEM((4,) + small, F32), pltpu.VMEM((4,) + small, F32),
                pltpu.VMEM(small, F32), pltpu.VMEM(small, F32), pltpu.VMEM(small, F32), pltpu.VMEM((EXT, half), F32),
                pltpu.VMEM((EXT, d), BF16), pltpu.VMEM((EXT, d), BF16),
                pltpu.SemaphoreType.DMA((17,)), pltpu.SemaphoreType.DMA((17,)), pltpu.SemaphoreType.DMA((8,)),
            ],
            compiler_params=pltpu.CompilerParams(collective_id=1, has_side_effects=True),
            name="scatter_sums",
        )(pm, pe, acc, z, gw)

    def device_step(x, slot_expert, w1, w3, w2, assign, wr, w1s, w3s, w2s):
        d = x.shape[1]
        at = jnp.concatenate([assign.T, jnp.full((2, assign.shape[0]), -1, I32)], axis=0)
        se = slot_expert.reshape(1, -1)

        def body(carry):
            r, _, acc = carry
            rnd = jnp.full((8, 128), r.astype(F32))
            xm, xe, wm, we, own, gw, z, nr = gather(x, at, se, wr, rnd, w1s, w3s, w2s)
            pm, pe = experts(own, slot_expert, xm.reshape(-1, d), xe.reshape(-1, d), wm, we, w1, w3, w2)
            acc = scatter(pm.reshape(8, 128, d), pe.reshape(8, EXT, d), acc, z, gw)
            return r + 1, nr[0, 0].astype(I32), acc

        carry = (jnp.int32(0), jnp.int32(1), jnp.zeros(x.shape, F32))
        out = lax.while_loop(lambda s: s[0] < s[1], body, carry)[2]
        return out.astype(BF16)

    tok = P(("dp", "ep"), None)
    slot = P("ep", None, None)
    return jax.shard_map(device_step, mesh=mesh,
                         in_specs=(tok, P(), slot, slot, slot, tok, P(), P(), P(), P()),
                         out_specs=tok, check_vma=False)
```

```python
import functools

import jax
import jax.numpy as jnp
from jax import lax
from jax.experimental import pallas as pl
from jax.experimental.pallas import tpu as pltpu
from jax.sharding import PartitionSpec as P

ROUTE_SCALE = 2.5
MESH = pl.DeviceIdType.MESH
NUM_EXPERTS = 64
EXT = 64
UNIT = 128
PIECES = 2
NBUF = 6
MAXENT = 16
GROUP = 16
TILES = 160
TILE = 16
F32, BF16, I32 = jnp.float32, jnp.bfloat16, jnp.int32


def dims():
    me = lax.axis_index("ep")
    c, y, z, h = me % 2, (me // 2) % 2, (me // 4) % 2, me // 8
    sib = me + 1 - 2 * c
    yn = me + 2 - 4 * y
    zn = me + 4 - 8 * z
    mir = me + 8 - 16 * h
    first = yn + c * (zn - yn)
    second = zn + c * (yn - zn)
    diag = yn + zn - me
    return me, c, h, sib, yn, zn, mir, first, second, diag


def barrier(peers):
    sem = pltpu.get_barrier_semaphore()
    for peer in peers:
        pl.semaphore_signal(sem, inc=1, device_id=peer, device_id_type=MESH)
    pl.semaphore_wait(sem, len(peers))


def dot(a, b, ca=1, cb=0):
    return lax.dot_general(a, b, (((ca,), (cb,)), ((), ())), preferred_element_type=F32)


def split3(v):
    hi = v.astype(BF16)
    rest = v - hi.astype(F32)
    mid = rest.astype(BF16)
    lo = (rest - mid.astype(F32)).astype(BF16)
    return hi, mid, lo


def gather_kernel(x_ref, at_ref, se_ref, rnd_ref, wr_ref, w1_hbm, w3_hbm, w2_hbm,
                  xm_out, xe_out, wm_out, we_out, own_out, gw_out, z_out, nr_out,
                  xs, xes, wms, wes, xcr, ecr, xsnd, esnd, wsnd, cand_s, own_s, flag_s, frecv,
                  w1s, w3s, w2s, ssem, rsem, lsem):
    me, c, h, sib, yn, zn, mir, first, second, diag = dims()
    dp = lax.axis_index("dp")
    qm, qf, qs, qg = me % 8, first % 8, second % 8, diag % 8
    loads = [pltpu.make_async_copy(a, b, lsem.at[i]) for i, (a, b) in
             enumerate(((w1_hbm, w1s), (w3_hbm, w3s), (w2_hbm, w2s)))]
    for cp in loads:
        cp.start()
    barrier([{"ep": sib}, {"ep": yn}, {"ep": zn}, {"ep": mir}, {"dp": 1 - dp}])

    def rcopy(src, dst, i, dev):
        return pltpu.make_async_remote_copy(src_ref=src, dst_ref=dst, send_sem=ssem.at[i], recv_sem=rsem.at[i],
                                            device_id=dev, device_id_type=MESH)

    def spread(own, buf, base, one, two):
        ep = lambda d: {"ep": d}
        q1, q2 = one % 8, two % 8
        return [rcopy(own, buf.at[qm], base, ep(one)), rcopy(own, buf.at[qm], base + 1, ep(two)),
                rcopy(own, buf.at[qm], base + 2, ep(sib)), rcopy(buf.at[q1], buf.at[q1], base + 3, ep(two)),
                rcopy(buf.at[q1], buf.at[q1], base + 4, ep(sib)), rcopy(buf.at[q2], buf.at[q2], base + 5, ep(sib)),
                rcopy(buf.at[qg], buf.at[qg], base + 6, ep(sib))]

    parts = [pl.ds(i * (x_ref.shape[0] // PIECES), x_ref.shape[0] // PIECES) for i in range(PIECES)]
    ax = [spread(x_ref.at[r], xs.at[:, r], 45 + 7 * i, first, second) for i, r in enumerate(parts)]
    for i in range(2):
        ax[0][i].start()

    n_tok = x_ref.shape[0]
    n_slots = se_ref.shape[0]
    rnd = jnp.full((1, 1), rnd_ref[0], I32).astype(F32)
    first_round = jnp.where(rnd == 0.0, 1.0, 0.0)
    expert_of = se_ref[...].reshape(1, n_slots)
    eye = (lax.broadcasted_iota(I32, (NUM_EXPERTS, n_slots), 0) == expert_of).astype(F32)
    eye_bf = eye.astype(BF16)
    lane_slot = lax.broadcasted_iota(I32, (1, n_slots), 1)
    per_half = n_slots // 2
    here = jnp.where((lane_slot >= h * per_half) & (lane_slot < (h + 1) * per_half), 1.0, 0.0)
    avail = jnp.where(jnp.sum(eye * here, axis=1, keepdims=True) > 0.0, 1.0, 0.0)
    row_slot = lax.broadcasted_iota(I32, (n_slots, n_tok), 0)
    hot = jnp.concatenate([(row_slot == at_ref[k:k + 1, :]).astype(F32).astype(BF16) for k in range(6)], axis=1)
    picks_all = dot(eye_bf, hot)
    picks = [picks_all[:, k * n_tok:(k + 1) * n_tok] for k in range(6)]
    code = lax.broadcasted_iota(I32, (NUM_EXPERTS, n_tok), 0).astype(F32) + 1.0
    ids = [jnp.sum(p * code, axis=0, keepdims=True) for p in picks]
    miss = [jnp.sum(p * (1.0 - avail), axis=0, keepdims=True) for p in picks]
    none = jnp.zeros((2, n_tok), F32)
    id_all = jnp.concatenate(ids + [none], axis=0)
    miss_all = jnp.concatenate(miss + [none], axis=0)

    upper = (lax.broadcasted_iota(I32, (n_tok, n_tok), 0) < lax.broadcasted_iota(I32, (n_tok, n_tok), 1))
    before = dot(miss_all.astype(BF16), upper.astype(F32).astype(BF16))
    offset = -EXT * rnd
    count = jnp.zeros((1, 1), F32)
    row_ext = lax.broadcasted_iota(I32, (EXT, n_tok), 0).astype(F32)
    sels = []
    for k in range(6):
        sels.append(jnp.where((row_ext == before[k:k + 1, :] + offset) & (miss[k] > 0.0), 1.0, 0.0))
        mk = jnp.sum(miss[k], axis=1, keepdims=True)
        offset += mk
        count += mk
    take = functools.reduce(lambda a, b: a + b, sels)
    xsnd[...] = dot(take.astype(BF16), x_ref[...]).astype(BF16)
    piece = [pl.ds(i * (EXT // PIECES), EXT // PIECES) for i in range(PIECES)]
    cross = [rcopy(xsnd.at[r], xcr.at[r], 20 + i, {"ep": mir}) for i, r in enumerate(piece)]
    cross.append(rcopy(esnd, ecr, 19, {"ep": mir}))
    for cp in cross[:-1]:
        cp.start()
    codes = jnp.zeros((8, EXT), F32)
    for k in range(6):
        codes += dot(jnp.broadcast_to(ids[k], (8, n_tok)).astype(BF16), sels[k].astype(BF16), 1, 1)
    esnd[...] = jnp.concatenate([codes, jnp.zeros((8, 128 - EXT), F32)], axis=1)
    cross[-1].start()
    for a in ax[1:]:
        for i in range(2):
            a[i].start()
    for a in ax:
        a[2].start()

    gate = jax.nn.sigmoid(dot(wr_ref[...], x_ref[...], 1, 1))
    picked = gate * functools.reduce(lambda a, b: a + b, picks)
    total = jnp.sum(picked, axis=0, keepdims=True)
    weight = ROUTE_SCALE * picked / jnp.maximum(total, 1e-30)
    wk = [jnp.sum(p * weight, axis=0, keepdims=True) for p in picks]
    w_all = jnp.concatenate(wk + [none], axis=0) * (1.0 - miss_all) * first_round
    packed = jnp.concatenate([id_all, w_all], axis=0)
    wsnd[...] = packed
    wms[qm] = packed
    aw = spread(wsnd, wms, 7, first, second)
    for i in range(3):
        aw[i].start()
    gw_out[...] = functools.reduce(lambda a, b: a + b, [sel * w for sel, w in zip(sels, wk)])
    flag_s[0] = jnp.broadcast_to(jnp.floor((count + (EXT - 1)) * (1.0 / EXT)), (8, 128))
    steps = [rcopy(flag_s.at[i], frecv.at[i], 14 + i, d) for i, d in
             enumerate(({"dp": 1 - dp}, {"ep": sib}, {"ep": mir}, {"ep": zn}, {"ep": yn}))]
    steps[0].start()

    def vote(i):
        steps[i].wait()
        flag_s[i + 1] = jnp.maximum(flag_s[i], frecv[i])
        steps[i + 1].start()

    outs = []

    def put_out(src, dst, i):
        outs.append(pltpu.make_async_copy(src, dst, lsem.at[i]))
        outs[-1].start()

    put_out(x_ref, xm_out.at[qm], 3)

    slot_row = lax.broadcasted_iota(I32, (n_slots, 128), 0)
    lane_dev = lax.broadcasted_iota(I32, (n_slots, 128), 1)
    lo = (lane_dev + 8 * h) * (n_slots // 16)
    block = ((slot_row >= lo) & (slot_row < lo + n_slots // 16) & (lane_dev < 8)).astype(F32).astype(BF16)
    cand = jnp.where(dot(eye_bf, block) > 0.0, 1.0, 0.0)
    several = jnp.where(jnp.sum(cand, axis=1, keepdims=True) > 1.0, 1.0, 0.0)
    lane = lax.broadcasted_iota(I32, (1, 128), 1).astype(F32)
    block_key = jnp.where(cand > 0.0, jnp.broadcast_to(lane, cand.shape), 1e9)
    cand_s[0] = block_key
    there = jnp.where(jnp.sum(eye * (1.0 - here), axis=1, keepdims=True) > 0.0, 1.0, 2.0)
    cand_s[1] = jnp.broadcast_to(several * there, cand.shape)
    load0 = jnp.sum(cand * (1.0 - several) * there, axis=0, keepdims=True)

    def pick(e, load):
        key = cand_s[0, pl.ds(e, 1), :] + load * 256.0
        best = jnp.min(key, axis=1, keepdims=True)
        sel = jnp.where((key == best) & (key < 1e8), 1.0, 0.0)
        own_s[pl.ds(e, 1), :] = sel
        return load + sel * cand_s[1, pl.ds(e, 1), :]

    load1 = lax.fori_loop(0, NUM_EXPERTS // 2, pick, load0)
    vote(0)

    for a in ax + [aw]:
        a[0].wait_recv()
        a[3].start()
        a[4].start()
    for a in ax + [aw]:
        a[1].wait_recv()
        a[5].start()
    put_out(xs.at[qf], xm_out.at[qf], 4)
    put_out(xs.at[qs], xm_out.at[qs], 5)
    vote(1)
    lax.fori_loop(NUM_EXPERTS // 2, NUM_EXPERTS, pick, load1)
    mine = jnp.where(lax.broadcasted_iota(I32, (8, 128), 1) == qm, 1.0, 0.0)
    own = dot(mine.astype(BF16), own_s[...].astype(BF16), 1, 1)
    own_out[...] = jnp.concatenate([own, jnp.zeros((8, 128 - NUM_EXPERTS), F32)], axis=1).astype(I32)
    vote(2)

    ew = spread(ecr, wes, 24, zn, yn)
    ex = [spread(xcr.at[r], xes.at[:, r], 31 + 7 * i, zn, yn) for i, r in enumerate(piece)]
    for i, a in enumerate(ex):
        cross[i].wait_recv()
        for n in range(3):
            a[n].start()
    cross[-1].wait_recv()
    wes[qm] = ecr[...]
    for n in range(3):
        ew[n].start()
    put_out(xcr, xe_out.at[qm], 6)
    vote(3)

    for cp in loads:
        cp.wait()
    hg = dot(x_ref[...], w1s[...])
    hu = dot(x_ref[...], w3s[...])
    act = (jax.nn.silu(hg) * hu).astype(BF16)
    z_out[...] = dot(act, w2s[...]) * first_round

    for a in ex + [ew]:
        a[0].wait_recv()
        a[3].start()
        a[4].start()
    for a in ex + [ew]:
        a[1].wait_recv()
        a[5].start()
    put_out(xes.at[zn % 8], xe_out.at[zn % 8], 7)
    put_out(xes.at[yn % 8], xe_out.at[yn % 8], 8)
    for a in ax + [aw]:
        a[3].wait_recv()
        a[6].start()
    put_out(xs.at[qg], xm_out.at[qg], 9)
    for n, i in enumerate((2, 4, 5, 6)):
        for a in ax + [aw]:
            a[i].wait_recv()
        q = (sib % 8, qs + 1 - 2 * c, qf + 1 - 2 * c, qg + 1 - 2 * c)[n]
        put_out(xs.at[q], xm_out.at[q], 10 + n)
    steps[4].wait()
    nr_out[...] = jnp.maximum(flag_s[4], frecv[4])[0:1, 0:1].astype(I32)
    for a in ex + [ew]:
        a[3].wait_recv()
        a[6].start()
    put_out(xes.at[qg], xe_out.at[qg], 14)
    for n, i in enumerate((2, 4, 5, 6)):
        for a in ex + [ew]:
            a[i].wait_recv()
        q = (sib % 8, zn % 8 + 1 - 2 * c, yn % 8 + 1 - 2 * c, qg + 1 - 2 * c)[n]
        put_out(xes.at[q], xe_out.at[q], 15 + n)
    put_out(wms, wm_out, 19)
    put_out(wes, we_out, 20)
    for a in [aw, ew, cross] + ax + ex:
        for cp in a:
            cp.wait_send()
    for cp in outs:
        cp.wait()


def expert_kernel(own_ref, se_ref, xm_hbm, xe_hbm, wm_ref, we_ref, w1_hbm, w3_hbm, w2_hbm, pm_out, pe_out,
                  xv, wrow, rank, pv, pev, obuf, kb, startv, starts, b1, b3, b2, slots, experts, seen, ent_e, ent_u, ent_i,
                  tile_e, tile_row, tile_rank, n_tiles, wsem, xsem, osem):
    me = lax.axis_index("ep")
    n_local = w1_hbm.shape[0]
    n_main, n_ext = 8 * 128, 8 * EXT
    n_tok = n_main + n_ext
    n_blk = n_tok // 128
    xl = [pltpu.make_async_copy(xm_hbm, xv.at[pl.ds(0, n_main)], xsem.at[0]),
          pltpu.make_async_copy(xe_hbm, xv.at[pl.ds(n_main, n_ext)], xsem.at[1])]
    for cp in xl:
        cp.start()

    def clear(e, carry):
        seen[e] = 0
        return carry

    lax.fori_loop(0, NUM_EXPERTS, clear, 0)

    def listing(s, n):
        e = se_ref[me * n_local + s]
        use = (own_ref[0, e] == 1) & (seen[e] == 0)

        @pl.when(use)
        def _():
            slots[n] = s
            experts[n] = e
            seen[e] = 1
        return jnp.where(use, n + 1, n)

    n_act = lax.fori_loop(0, n_local, listing, 0)

    def fetch(i):
        s, b = slots[i], lax.rem(i, NBUF)
        return [pltpu.make_async_copy(w1_hbm.at[s], b1.at[b], wsem.at[0, b]),
                pltpu.make_async_copy(w3_hbm.at[s], b3.at[b], wsem.at[1, b]),
                pltpu.make_async_copy(w2_hbm.at[s], b2.at[b], wsem.at[2, b])]

    def start(i):
        @pl.when(i < n_act)
        def _():
            for cp in fetch(i):
                cp.start()

    for i in range(NBUF):
        start(i)

    upper = (lax.broadcasted_iota(I32, (128, 128), 0) < lax.broadcasted_iota(I32, (128, 128), 1))
    upper = upper.astype(F32).astype(BF16)
    lane = lax.broadcasted_iota(I32, (NUM_EXPERTS, 128), 1)
    code = lax.broadcasted_iota(I32, (NUM_EXPERTS, 128), 0).astype(F32) + 1.0
    run = jnp.zeros((NUM_EXPERTS, 1), F32)
    table = jnp.zeros((NUM_EXPERTS, 128), F32)
    for j in range(n_blk):
        if j < 8:
            blk = wm_ref[j]
            w = jnp.zeros((NUM_EXPERTS, 128), F32)
            for k in range(6):
                w += jnp.where(code == blk[k:k + 1, :], blk[8 + k:9 + k, :], 0.0)
        else:
            ids = jnp.concatenate([we_ref[2 * (j - 8)][:1, :EXT], we_ref[2 * (j - 8) + 1][:1, :EXT]], axis=1)
            w = jnp.where(code == ids, 1.0, 0.0)
        mask = jnp.where(w != 0.0, 1.0, 0.0)
        pos = dot(mask.astype(BF16), upper) + run
        run += jnp.sum(mask, axis=1, keepdims=True)
        table += jnp.where(lane == j + 1, run, 0.0)
        rank[j] = jnp.where(mask > 0.0, pos, -1.0)
        wrow[j] = w
    startv[...] = table.astype(I32)
    tc = pltpu.make_async_copy(startv, starts, xsem.at[2])
    tc.start()
    tc.wait()

    def list_units(i, n):
        e = experts[i]
        units = (starts[e, n_blk] + UNIT - 1) // UNIT

        def put(u, n):
            ent_e[n] = e
            ent_u[n] = u
            ent_i[n] = i
            return n + 1
        return lax.fori_loop(0, units, put, n)

    n_all = lax.fori_loop(0, n_act, list_units, 0)
    for cp in xl:
        cp.wait()

    def out_copies(j):
        if j < 8:
            return pltpu.make_async_copy(pv.at[pl.ds(j * 128, 128)], pm_out.at[pl.ds(j * 128, 128)], osem.at[j])
        return pltpu.make_async_copy(pev.at[pl.ds((j - 8) * 128, 128)], pe_out.at[pl.ds((j - 8) * 128, 128)], osem.at[j])

    def finish(j):
        if j >= 8:
            pev[(j - 8) * 128:(j - 7) * 128, :] = pv[j * 128:(j + 1) * 128, :].astype(BF16)
        out_copies(j).start()

    def flush(first, n_ent, last):
        for j in range(n_blk):
            n_tiles[j] = 0

        def list_tiles(g, carry):
            e, u = ent_e[first + g], ent_u[first + g] * UNIT
            hi = jnp.clip(starts[e, 0] - u, 0, UNIT)
            for j in range(n_blk):
                lo, hi = hi, jnp.clip(starts[e, j + 1] - u, 0, UNIT)
                k0 = lo // TILE
                some = hi > lo
                k1 = jnp.where(some, (hi - 1) // TILE + 1, k0)
                t = n_tiles[j]

                def put(k, t):
                    tile_e[j * TILES + t] = e
                    tile_row[j * TILES + t] = g * UNIT + k * TILE
                    tile_rank[j * TILES + t] = u + k * TILE

                put(k0, t)
                put(k0 + 1, t + 1)
                n_tiles[j] = t + k1 - k0

                @pl.when(k1 > k0 + 2)
                def _():
                    lax.fori_loop(2, k1 - k0, lambda k, _: put(k0 + k, t + k), None)
            return carry

        lax.fori_loop(0, n_ent, list_tiles, 0)
        for j in range(n_blk):
            n_tile = n_tiles[j]

            def one_pass(p, carry, j=j, n_tile=n_tile):
                parts = []
                for g in range(GROUP):
                    t = p * GROUP + g
                    live = t < n_tile
                    e = jnp.where(live, tile_e[j * TILES + t], 0)
                    at = jnp.where(live, tile_row[j * TILES + t], 0)
                    base = jnp.where(live, tile_rank[j * TILES + t], -1000)
                    kb[g * TILE:(g + 1) * TILE, :] = obuf[pl.ds(pl.multiple_of(at, TILE), TILE), :]
                    rows = lax.broadcasted_iota(I32, (TILE, 128), 0) + base
                    hit = rows.astype(F32) == rank[j, pl.ds(e, 1), :]
                    parts.append(jnp.where(hit, wrow[j, pl.ds(e, 1), :], 0.0))
                st = jnp.transpose(jnp.concatenate(parts, axis=0))
                res = dot(jnp.concatenate(split3(st), axis=0), kb[...])
                res = res[:128] + res[128:256] + res[256:]
                fresh = (first == 0) & (p == 0)

                @pl.when(fresh)
                def _():
                    pv[j * 128:(j + 1) * 128, :] = res

                @pl.when(jnp.logical_not(fresh))
                def _():
                    pv[j * 128:(j + 1) * 128, :] += res
                return carry

            @pl.when((first == 0) & (n_tile == 0))
            def _():
                pv[j * 128:(j + 1) * 128, :] = jnp.zeros((128, pv.shape[1]), F32)
            lax.fori_loop(0, (n_tile + GROUP - 1) // GROUP, one_pass, 0)

            @pl.when(last)
            def _():
                finish(j)

    def wait_for(k, carry):
        for cp in fetch(k):
            cp.wait()
        return carry

    def batch(bt, nxt):
        first = bt * MAXENT
        n_ent = jnp.minimum(n_all - first, MAXENT)

        def collect(q, carry):
            es = [jnp.minimum(q * 4 + g, n_ent - 1) + first for g in range(4)]
            ext = functools.reduce(jnp.logical_or, [starts[ent_e[n], n_blk] > starts[ent_e[n], 8] for n in es])

            def take(width):
                sel = []
                for n in es:
                    rows = (lax.broadcasted_iota(I32, (UNIT, 128), 0) + ent_u[n] * UNIT).astype(F32)
                    e = ent_e[n]
                    sel.append(jnp.concatenate([jnp.where(rows == rank[j, pl.ds(e, 1), :], 1.0, 0.0).astype(BF16)
                                                for j in range(width // 128)], axis=1))
                got = dot(jnp.concatenate(sel, axis=0), xv[:width, :])
                obuf[pl.ds(pl.multiple_of(q * 4 * UNIT, 4 * UNIT), 4 * UNIT), :] = got.astype(BF16)

            @pl.when(ext)
            def _():
                take(n_tok)

            @pl.when(jnp.logical_not(ext))
            def _():
                take(n_main)
            return carry

        lax.fori_loop(0, (n_ent + 3) // 4, collect, 0)

        def run_ffn(k, nxt):
            i = ent_i[first + k]

            def settle(k, carry):
                wait_for(k, carry)

                @pl.when(k < i)
                def _():
                    start(k + NBUF)
                return carry
            lax.fori_loop(nxt, i + 1, settle, 0)
            b = lax.rem(i, NBUF)
            two = (k + 1 < n_ent) & (ent_i[first + k + 1] == i)

            def ffn(n):
                rows = pl.ds(pl.multiple_of(k * UNIT, UNIT), n)
                xg = obuf[rows, :]
                act = (jax.nn.silu(dot(xg, b1[b])) * dot(xg, b3[b])).astype(BF16)
                obuf[rows, :] = dot(act, b2[b]).astype(BF16)

            @pl.when(two)
            def _():
                ffn(2 * UNIT)

            @pl.when(jnp.logical_not(two))
            def _():
                ffn(UNIT)
            end = k + jnp.where(two, 2, 1)

            @pl.when((first + end == n_all) | (ent_i[first + end] != i))
            def _():
                start(i + NBUF)
            return end, jnp.maximum(nxt, i + 1)

        nxt = lax.while_loop(lambda s: s[0] < n_ent, lambda s: run_ffn(*s), (0, nxt))[1]
        flush(first, n_ent, first + n_ent == n_all)
        return nxt

    nxt = lax.fori_loop(0, (n_all + MAXENT - 1) // MAXENT, batch, 0)

    def drain(k, carry):
        wait_for(k, carry)
        start(k + NBUF)
        return carry

    lax.fori_loop(nxt, n_act, drain, 0)

    @pl.when(n_all == 0)
    def _():
        pv[...] = jnp.zeros_like(pv)
        for j in range(n_blk):
            finish(j)
    for j in range(n_blk):
        out_copies(j).wait()


def scatter_kernel(pm_hbm, pe_hbm, z_ref, gw_ref, y_ref,
                   out_ref, mo, md, mrg, mrf, mrs, mfin, eo, ed, erg, erf, ers, gsib, ecr, ssem, rsem, lsem):
    me, c, h, sib, yn, zn, mir, first, second, diag = dims()
    cols = mo.shape[-1]
    mine = pl.ds(pl.multiple_of(c * cols, 128), cols)
    theirs = pl.ds(pl.multiple_of((1 - c) * cols, 128), cols)
    local, peer = [], []
    for base, (src, own, got, chips, swap) in ((0, (pe_hbm, eo, ed, (diag, yn, zn, me), (0, 1, 2, 3))),
                                               (4, (pm_hbm, mo, md, (diag, first, second, me), (0, 2, 1, 3)))):
        for i in range(4):
            rows = pl.ds(2 * ((chips[i] % 8) // 2), 2)
            sib_rows = pl.ds(2 * ((chips[swap[i]] % 8) // 2), 2)
            local.append(pltpu.make_async_copy(src.at[rows, :, mine], own.at[i], lsem.at[base + i]))
            peer.append(pltpu.make_async_remote_copy(
                src_ref=src.at[sib_rows, :, theirs], dst_ref=got.at[i], send_sem=ssem.at[base + i],
                recv_sem=rsem.at[base + i], device_id={"ep": sib}, device_id_type=MESH))
    for i in (0, 4, 1, 5, 2, 6, 3, 7):
        local[i].start()
    barrier([{"ep": sib}, {"ep": yn}, {"ep": zn}, {"ep": mir}])
    for i in (0, 4, 1, 5, 2, 6, 3, 7):
        peer[i].start()

    def rcopy(src, dst, i, dev):
        return pltpu.make_async_remote_copy(src_ref=src, dst_ref=dst, send_sem=ssem.at[i], recv_sem=rsem.at[i],
                                            device_id={"ep": dev}, device_id_type=MESH)

    eg, ef, es = rcopy(eo.at[0], erg, 8, yn), rcopy(eo.at[1], erf, 9, yn), rcopy(eo.at[2], ers, 10, zn)
    back = rcopy(eo.at[3], ecr, 11, mir)
    gshare = rcopy(gw_ref, gsib, 12, sib)
    order = (1 - c, c)
    mg = [rcopy(mo.at[0, b], mrg.at[b], 13 + n, first) for n, b in enumerate(order)]
    ms = [rcopy(mo.at[2, b], mrs.at[b], 15 + n, second) for n, b in enumerate(order)]
    mf = rcopy(mo.at[1], mrf, 17, first)
    mfinal = rcopy(mo.at[3, 1 - c], mfin, 18, sib)

    def joined(own, got, i, base):
        local[base + i].wait()
        peer[base + i].wait_recv()
        own[i] = own[i] + got[i]

    joined(eo, ed, 0, 0)
    eg.start()
    joined(mo, md, 0, 4)
    mg[0].start()
    joined(eo, ed, 1, 0)
    ef.start()
    mg[1].start()
    joined(eo, ed, 2, 0)
    joined(eo, ed, 3, 0)
    gshare.start()
    eg.wait_recv()
    eo[2] = eo[2] + erg[...]
    es.start()
    joined(mo, md, 1, 4)
    mf.start()
    joined(mo, md, 2, 4)
    mg[0].wait_recv()
    mo[2, 1 - c] = mo[2, 1 - c] + mrg[1 - c]
    ms[0].start()
    ef.wait_recv()
    es.wait_recv()
    eo[3] = eo[3] + erf[...] + ers[...]
    back.start()
    joined(mo, md, 3, 4)
    out_ref[...] = z_ref[...]
    mg[1].wait_recv()
    mo[2, c] = mo[2, c] + mrg[c]
    ms[1].start()
    mf.wait_recv()
    mo[3] = mo[3] + mrf[...]
    gshare.wait_recv()
    back.wait_recv()
    for b, g in ((c, gw_ref), (1 - c, gsib)):
        for part in split3(g[...]):
            mo[3, b] += dot(part, ecr[b], 0, 0)
    ms[0].wait_recv()
    mo[3, 1 - c] = mo[3, 1 - c] + mrs[1 - c]
    mfinal.start()
    ms[1].wait_recv()
    out_ref[:, mine] += mo[3, c] + mrs[c]
    mfinal.wait_recv()
    out_ref[:, theirs] += mfin[...]
    y_ref[...] = out_ref[...].astype(y_ref.dtype)
    for cp in peer + mg + ms + [eg, ef, es, back, gshare, mf, mfinal]:
        cp.wait_send()


def solution(mesh):
    any_space = pl.BlockSpec(memory_space=pl.ANY)
    vmem = pl.BlockSpec(memory_space=pltpu.VMEM)
    smem = pl.BlockSpec(memory_space=pltpu.SMEM)
    sds = jax.ShapeDtypeStruct

    def gather(x, at, se, rnd, wr, w1, w3, w2):
        d, ff = w1.shape
        return pl.pallas_call(
            gather_kernel,
            out_shape=(sds((8, 128, d), BF16), sds((8, EXT, d), BF16), sds((8, 16, 128), F32),
                       sds((8, 8, 128), F32), sds((8, 128), I32), sds((EXT, 128), F32),
                       sds((128, d), F32), sds((1, 1), I32)),
            in_specs=[vmem, vmem, vmem, smem, vmem] + [any_space] * 3,
            out_specs=(any_space,) * 4 + (vmem,) * 4,
            scratch_shapes=[
                pltpu.VMEM((8, 128, d), BF16), pltpu.VMEM((8, EXT, d), BF16),
                pltpu.VMEM((8, 16, 128), F32), pltpu.VMEM((8, 8, 128), F32),
                pltpu.VMEM((EXT, d), BF16), pltpu.VMEM((8, 128), F32),
                pltpu.VMEM((EXT, d), BF16), pltpu.VMEM((8, 128), F32), pltpu.VMEM((16, 128), F32),
                pltpu.VMEM((2, NUM_EXPERTS, 128), F32), pltpu.VMEM((NUM_EXPERTS, 128), F32),
                pltpu.VMEM((5, 8, 128), F32), pltpu.VMEM((5, 8, 128), F32),
                pltpu.VMEM((d, ff), BF16), pltpu.VMEM((d, ff), BF16), pltpu.VMEM((ff, d), BF16),
                pltpu.SemaphoreType.DMA((60,)), pltpu.SemaphoreType.DMA((60,)), pltpu.SemaphoreType.DMA((21,)),
            ],
            compiler_params=pltpu.CompilerParams(collective_id=0, has_side_effects=True),
            name="gather_rows",
        )(x, at, se, rnd, wr, w1, w3, w2)

    def experts(own, se, xm, xe, wm, we, w1, w3, w2):
        _, d, ff = w1.shape
        n_tok = 8 * (128 + EXT)
        return pl.pallas_call(
            expert_kernel,
            out_shape=(sds((8 * 128, d), F32), sds((8 * EXT, d), BF16)),
            in_specs=[smem, smem, any_space, any_space, vmem, vmem] + [any_space] * 3,
            out_specs=(any_space, any_space),
            scratch_shapes=[
                pltpu.VMEM((n_tok, d), BF16), pltpu.VMEM((n_tok // 128, NUM_EXPERTS, 128), F32), pltpu.VMEM((n_tok // 128, NUM_EXPERTS, 128), F32),
                pltpu.VMEM((n_tok, d), F32), pltpu.VMEM((8 * EXT, d), BF16), pltpu.VMEM((MAXENT * UNIT, d), BF16),
                pltpu.VMEM((GROUP * TILE, d), BF16),
                pltpu.VMEM((NUM_EXPERTS, 128), I32), pltpu.SMEM((NUM_EXPERTS, 128), I32),
                pltpu.VMEM((NBUF, d, ff), BF16), pltpu.VMEM((NBUF, d, ff), BF16), pltpu.VMEM((NBUF, ff, d), BF16),
                pltpu.SMEM((32,), I32), pltpu.SMEM((32,), I32), pltpu.SMEM((NUM_EXPERTS,), I32),
                pltpu.SMEM((384,), I32), pltpu.SMEM((384,), I32), pltpu.SMEM((384,), I32),
                pltpu.SMEM((12 * TILES,), I32), pltpu.SMEM((12 * TILES,), I32), pltpu.SMEM((12 * TILES,), I32),
                pltpu.SMEM((16,), I32),
                pltpu.SemaphoreType.DMA((3, NBUF)), pltpu.SemaphoreType.DMA((3,)), pltpu.SemaphoreType.DMA((12,)),
            ],
            name="expert_rows",
        )(own, se, xm, xe, wm, we, w1, w3, w2)

    def scatter(pm, pe, z, gw, last):
        d = z.shape[1]
        half = d // 2
        big, small = (2, 128, half), (2, EXT, half)
        return pl.pallas_call(
            scatter_kernel,
            out_shape=sds((128, d), F32),
            in_specs=[any_space, any_space, vmem, vmem],
            out_specs=vmem,
            scratch_shapes=[
                pltpu.VMEM((128, d), F32),
                pltpu.VMEM((4,) + big, F32), pltpu.VMEM((4,) + big, F32),
                pltpu.VMEM(big, F32), pltpu.VMEM(big, F32), pltpu.VMEM(big, F32), pltpu.VMEM((128, half), F32),
                pltpu.VMEM((4,) + small, BF16), pltpu.VMEM((4,) + small, BF16),
                pltpu.VMEM(small, BF16), pltpu.VMEM(small, BF16), pltpu.VMEM(small, BF16), pltpu.VMEM((EXT, 128), F32),
                pltpu.VMEM(small, BF16),
                pltpu.SemaphoreType.DMA((20,)), pltpu.SemaphoreType.DMA((20,)), pltpu.SemaphoreType.DMA((8,)),
            ],
            compiler_params=pltpu.CompilerParams(collective_id=1 if last else 2, has_side_effects=True),
            name="scatter_sums" if last else "scatter_more",
        )(pm, pe, z, gw)

    def device_step(x, slot_expert, w1, w3, w2, assign, wr, w1s, w3s, w2s):
        d = x.shape[1]
        rows_of = lambda a: a.reshape(-1, d)

        def gathered(r):
            return gather(x, assign.T, slot_expert, r.reshape(1), wr.T, w1s, w3s, w2s)

        def summed(parts):
            xm, xe, wm, we, own = parts
            pm, pe = experts(own, slot_expert, rows_of(xm), rows_of(xe), wm, we, w1, w3, w2)
            return pm.reshape(8, 128, d), pe.reshape(8, EXT, d)

        def again(carry):
            r, n, z = carry
            *parts, gw, _, _ = gathered(r)
            return r + 1, n, scatter(*summed(parts), z, gw, False)

        *parts, gw, z, nr = gathered(jnp.int32(0))
        z = lax.while_loop(lambda s: s[0] < s[1], again, (jnp.int32(1), nr.reshape(()), z))[2]
        return scatter(*summed(parts), z, gw, True).astype(BF16)

    tok = P(("dp", "ep"), None)
    slot = P("ep", None, None)
    return jax.shard_map(device_step, mesh=mesh,
                         in_specs=(tok, P(), slot, slot, slot, tok, P(), P(), P(), P()),
                         out_specs=tok, check_vma=False)
```

```python
import functools

import jax
import jax.numpy as jnp
from jax import lax
from jax.experimental import pallas as pl
from jax.experimental.pallas import tpu as pltpu
from jax.sharding import PartitionSpec as P

ROUTE_SCALE = 2.5
LANES, PEERS, CHIPS = 128, 8, 4
ZERO, ONE = 0.0, 1.0
MESH = pl.DeviceIdType.MESH
NUM_EXPERTS = 64
EXT = 64
UNIT = LANES
PIECES = 2
NBUF = 6
MAXENT = 15
GROUP = 16
TILES = 160
TILE_BITS = CHIPS
TILE = 1 << TILE_BITS
TAKE = 3
F32, BF16, I32 = jnp.float32, jnp.bfloat16, jnp.int32


def dims():
    me = lax.axis_index("ep")
    c, y, z, h = me % 2, (me // 2) % 2, (me // CHIPS) % 2, me // PEERS
    sib = me + 1 - 2 * c
    yn = me + 2 - CHIPS * y
    zn = me + CHIPS - PEERS * z
    mir = me + PEERS - 16 * h
    first = yn + c * (zn - yn)
    second = zn + c * (yn - zn)
    diag = yn + zn - me
    return me, c, h, sib, yn, zn, mir, first, second, diag


def barrier(peers):
    sem = pltpu.get_barrier_semaphore()
    for peer in peers:
        pl.semaphore_signal(sem, inc=1, device_id=peer, device_id_type=MESH)
    pl.semaphore_wait(sem, len(peers))


def dot(a, b, ca=1, cb=0):
    return lax.dot_general(a, b, (((ca,), (cb,)), ((), ())), preferred_element_type=F32)


def split3(v):
    hi = v.astype(BF16)
    rest = v - hi.astype(F32)
    mid = rest.astype(BF16)
    lo = (rest - mid.astype(F32)).astype(BF16)
    return hi, mid, lo


def gather_kernel(x_ref, at_ref, se_ref, rnd_ref, wr_ref, w1_hbm, w3_hbm, w2_hbm,
                  xm_out, xe_out, wm_out, we_out, own_out, gw_out, z_out, nr_out,
                  xs, xes, wms, wes, xcr, ecr, xsnd, esnd, wsnd, cand_s, own_s, flag_s, frecv,
                  w1s, w3s, w2s, ssem, rsem, lsem):
    me, c, h, sib, yn, zn, mir, first, second, diag = dims()
    dp = lax.axis_index("dp")
    qm, qf, qs, qg = me % PEERS, first % PEERS, second % PEERS, diag % PEERS
    loads = [pltpu.make_async_copy(a, b, lsem.at[i]) for i, (a, b) in
             enumerate(((w1_hbm, w1s), (w3_hbm, w3s), (w2_hbm, w2s)))]
    for cp in loads:
        cp.start()
    barrier([{"ep": sib}, {"ep": yn}, {"ep": zn}, {"ep": mir}, {"dp": 1 - dp}])

    def rcopy(src, dst, i, dev):
        return pltpu.make_async_remote_copy(src_ref=src, dst_ref=dst, send_sem=ssem.at[i], recv_sem=rsem.at[i],
                                            device_id=dev, device_id_type=MESH)

    def spread(own, buf, base, one, two):
        ep = lambda d: {"ep": d}
        q1, q2 = one % PEERS, two % PEERS
        return [rcopy(own, buf.at[qm], base, ep(one)), rcopy(own, buf.at[qm], base + 1, ep(two)),
                rcopy(own, buf.at[qm], base + 2, ep(sib)), rcopy(buf.at[q1], buf.at[q1], base + 3, ep(two)),
                rcopy(buf.at[q1], buf.at[q1], base + CHIPS, ep(sib)), rcopy(buf.at[q2], buf.at[q2], base + 5, ep(sib)),
                rcopy(buf.at[qg], buf.at[qg], base + 6, ep(sib))]

    parts = [pl.ds(i * (x_ref.shape[0] // PIECES), x_ref.shape[0] // PIECES) for i in range(PIECES)]
    ax = [spread(x_ref.at[r], xs.at[:, r], 45 + 7 * i, first, second) for i, r in enumerate(parts)]
    for i in range(2):
        ax[0][i].start()

    n_tok = x_ref.shape[0]
    n_slots = se_ref.shape[0]
    rnd = jnp.full((1, 1), rnd_ref[0], I32).astype(F32)
    first_round = jnp.where(rnd == ZERO, ONE, ZERO)
    expert_of = se_ref[...].reshape(1, n_slots)
    eye = (lax.broadcasted_iota(I32, (NUM_EXPERTS, n_slots), 0) == expert_of).astype(F32)
    eye_bf = eye.astype(BF16)
    lane_slot = lax.broadcasted_iota(I32, (1, n_slots), 1)
    per_half = n_slots // 2
    here = jnp.where((lane_slot >= h * per_half) & (lane_slot < (h + 1) * per_half), ONE, ZERO)
    avail = jnp.where(jnp.sum(eye * here, axis=1, keepdims=True) > ZERO, ONE, ZERO)
    row_slot = lax.broadcasted_iota(I32, (n_slots, n_tok), 0)
    hot = jnp.concatenate([(row_slot == at_ref[k:k + 1, :]).astype(F32).astype(BF16) for k in range(6)], axis=1)
    picks_all = dot(eye_bf, hot)
    picks = [picks_all[:, k * n_tok:(k + 1) * n_tok] for k in range(6)]
    code = lax.broadcasted_iota(I32, (NUM_EXPERTS, n_tok), 0).astype(F32) + ONE
    ids = [jnp.sum(p * code, axis=0, keepdims=True) for p in picks]
    miss = [jnp.sum(p * (ONE - avail), axis=0, keepdims=True) for p in picks]
    none = jnp.zeros((2, n_tok), F32)
    id_all = jnp.concatenate(ids + [none], axis=0)
    miss_all = jnp.concatenate(miss + [none], axis=0)

    upper = (lax.broadcasted_iota(I32, (n_tok, n_tok), 0) < lax.broadcasted_iota(I32, (n_tok, n_tok), 1))
    before = dot(miss_all.astype(BF16), upper.astype(F32).astype(BF16))
    offset = -EXT * rnd
    count = jnp.zeros((1, 1), F32)
    row_ext = lax.broadcasted_iota(I32, (EXT, n_tok), 0).astype(F32)
    sels = []
    for k in range(6):
        sels.append(jnp.where((row_ext == before[k:k + 1, :] + offset) & (miss[k] > ZERO), ONE, ZERO))
        mk = jnp.sum(miss[k], axis=1, keepdims=True)
        offset += mk
        count += mk
    take = functools.reduce(lambda a, b: a + b, sels)
    xsnd[...] = dot(take.astype(BF16), x_ref[...]).astype(BF16)
    piece = [pl.ds(i * (EXT // PIECES), EXT // PIECES) for i in range(PIECES)]
    cross = [rcopy(xsnd.at[r], xcr.at[r], 20 + i, {"ep": mir}) for i, r in enumerate(piece)]
    cross.append(rcopy(esnd, ecr, 19, {"ep": mir}))
    for cp in cross[:-1]:
        cp.start()
    codes = jnp.zeros((PEERS, EXT), F32)
    for k in range(6):
        codes += dot(jnp.broadcast_to(ids[k], (PEERS, n_tok)).astype(BF16), sels[k].astype(BF16), 1, 1)
    esnd[...] = jnp.concatenate([codes, jnp.zeros((PEERS, LANES - EXT), F32)], axis=1)
    cross[-1].start()
    for a in ax[1:]:
        for i in range(2):
            a[i].start()
    for a in ax:
        a[2].start()

    gate = jax.nn.sigmoid(dot(wr_ref[...], x_ref[...], 1, 1))
    picked = gate * functools.reduce(lambda a, b: a + b, picks)
    total = jnp.sum(picked, axis=0, keepdims=True)
    weight = ROUTE_SCALE * picked / jnp.maximum(total, 1e-30)
    wk = [jnp.sum(p * weight, axis=0, keepdims=True) for p in picks]
    w_all = jnp.concatenate(wk + [none], axis=0) * (ONE - miss_all) * first_round
    packed = jnp.concatenate([id_all, w_all], axis=0)
    wsnd[...] = packed
    wms[qm] = packed
    aw = spread(wsnd, wms, 7, first, second)
    for i in range(3):
        aw[i].start()
    gw_out[...] = functools.reduce(lambda a, b: a + b, [sel * w for sel, w in zip(sels, wk)])
    flag_s[0] = jnp.broadcast_to(jnp.floor((count + (EXT - 1)) * (ONE / EXT)), (PEERS, LANES))
    steps = [rcopy(flag_s.at[i], frecv.at[i], 14 + i, d) for i, d in
             enumerate(({"dp": 1 - dp}, {"ep": sib}, {"ep": mir}, {"ep": zn}, {"ep": yn}))]
    steps[0].start()

    def vote(i):
        steps[i].wait()
        flag_s[i + 1] = jnp.maximum(flag_s[i], frecv[i])
        steps[i + 1].start()

    outs = []

    def put_out(src, dst, i):
        outs.append(pltpu.make_async_copy(src, dst, lsem.at[i]))
        outs[-1].start()

    put_out(x_ref, xm_out.at[qm], 3)

    slot_row = lax.broadcasted_iota(I32, (n_slots, LANES), 0)
    lane_dev = lax.broadcasted_iota(I32, (n_slots, LANES), 1)
    lo = (lane_dev + PEERS * h) * (n_slots // 16)
    block = ((slot_row >= lo) & (slot_row < lo + n_slots // 16) & (lane_dev < PEERS)).astype(F32).astype(BF16)
    cand = jnp.where(dot(eye_bf, block) > ZERO, ONE, ZERO)
    several = jnp.where(jnp.sum(cand, axis=1, keepdims=True) > ONE, ONE, ZERO)
    lane = lax.broadcasted_iota(I32, (1, LANES), 1).astype(F32)
    block_key = jnp.where(cand > ZERO, jnp.broadcast_to(lane, cand.shape), 1e9)
    cand_s[0] = block_key
    there = jnp.where(jnp.sum(eye * (ONE - here), axis=1, keepdims=True) > ZERO, ONE, 2.0)
    cand_s[1] = jnp.broadcast_to(several * there, cand.shape)
    load0 = jnp.sum(cand * (ONE - several) * there, axis=0, keepdims=True)

    def pick(e, load):
        key = cand_s[0, pl.ds(e, 1), :] + load * 256.0
        best = jnp.min(key, axis=1, keepdims=True)
        sel = jnp.where((key == best) & (key < 1e8), ONE, ZERO)
        own_s[pl.ds(e, 1), :] = sel
        return load + sel * cand_s[1, pl.ds(e, 1), :]

    load1 = lax.fori_loop(0, NUM_EXPERTS // 2, pick, load0)
    vote(0)

    for a in ax + [aw]:
        a[0].wait_recv()
        a[3].start()
        a[CHIPS].start()
    for a in ax + [aw]:
        a[1].wait_recv()
        a[5].start()
    put_out(xs.at[qf], xm_out.at[qf], CHIPS)
    put_out(xs.at[qs], xm_out.at[qs], 5)
    vote(1)
    lax.fori_loop(NUM_EXPERTS // 2, NUM_EXPERTS, pick, load1)
    mine = jnp.where(lax.broadcasted_iota(I32, (PEERS, LANES), 1) == qm, ONE, ZERO)
    own = dot(mine.astype(BF16), own_s[...].astype(BF16), 1, 1)
    own_out[...] = jnp.concatenate([own, jnp.zeros((PEERS, LANES - NUM_EXPERTS), F32)], axis=1).astype(I32)
    vote(2)

    ew = spread(ecr, wes, 24, zn, yn)
    ex = [spread(xcr.at[r], xes.at[:, r], 31 + 7 * i, zn, yn) for i, r in enumerate(piece)]
    for i, a in enumerate(ex):
        cross[i].wait_recv()
        for n in range(3):
            a[n].start()
    cross[-1].wait_recv()
    wes[qm] = ecr[...]
    for n in range(3):
        ew[n].start()
    put_out(xcr, xe_out.at[qm], 6)
    vote(3)

    for cp in loads:
        cp.wait()
    hg = dot(x_ref[...], w1s[...])
    hu = dot(x_ref[...], w3s[...])
    act = (jax.nn.silu(hg) * hu).astype(BF16)
    z_out[...] = dot(act, w2s[...]) * first_round

    for a in ex + [ew]:
        a[0].wait_recv()
        a[3].start()
        a[CHIPS].start()
    for a in ex + [ew]:
        a[1].wait_recv()
        a[5].start()
    put_out(xes.at[zn % PEERS], xe_out.at[zn % PEERS], 7)
    put_out(xes.at[yn % PEERS], xe_out.at[yn % PEERS], PEERS)
    for a in ax + [aw]:
        a[3].wait_recv()
        a[6].start()
    put_out(xs.at[qg], xm_out.at[qg], 9)
    for n, i in enumerate((2, CHIPS, 5, 6)):
        for a in ax + [aw]:
            a[i].wait_recv()
        q = (sib % PEERS, qs + 1 - 2 * c, qf + 1 - 2 * c, qg + 1 - 2 * c)[n]
        put_out(xs.at[q], xm_out.at[q], 10 + n)
    steps[CHIPS].wait()
    nr_out[...] = jnp.maximum(flag_s[CHIPS], frecv[CHIPS])[0:1, 0:1].astype(I32)
    for a in ex + [ew]:
        a[3].wait_recv()
        a[6].start()
    put_out(xes.at[qg], xe_out.at[qg], 14)
    for n, i in enumerate((2, CHIPS, 5, 6)):
        for a in ex + [ew]:
            a[i].wait_recv()
        q = (sib % PEERS, zn % PEERS + 1 - 2 * c, yn % PEERS + 1 - 2 * c, qg + 1 - 2 * c)[n]
        put_out(xes.at[q], xe_out.at[q], 15 + n)
    put_out(wms, wm_out, 19)
    put_out(wes, we_out, 20)
    for a in [aw, ew, cross] + ax + ex:
        for cp in a:
            cp.wait_send()
    for cp in outs:
        cp.wait()


def expert_kernel(own_ref, se_ref, xm_hbm, xe_hbm, wm_ref, we_ref, w1_hbm, w3_hbm, w2_hbm, pm_out, pe_out,
                  xv, wrow, rank, pv, pev, obuf, kb, startv, starts, b1, b3, b2, slots, experts, seen, ent_e, ent_u, ent_i,
                  tile_e, tile_row, tile_rank, n_tiles, wsem, xsem, osem):
    me = lax.axis_index("ep")
    n_local = w1_hbm.shape[0]
    n_main, n_ext = PEERS * LANES, PEERS * EXT
    n_tok = n_main + n_ext
    n_blk = n_tok // LANES
    xl = [pltpu.make_async_copy(xm_hbm, xv.at[pl.ds(0, n_main)], xsem.at[0]),
          pltpu.make_async_copy(xe_hbm, xv.at[pl.ds(n_main, n_ext)], xsem.at[1])]
    for cp in xl:
        cp.start()

    def clear(e, carry):
        seen[e] = 0
        return carry

    lax.fori_loop(0, NUM_EXPERTS, clear, 0)

    def listing(s, n):
        e = se_ref[me * n_local + s]
        use = (own_ref[0, e] == 1) & (seen[e] == 0)

        @pl.when(use)
        def _():
            slots[n] = s
            experts[n] = e
            seen[e] = 1
        return jnp.where(use, n + 1, n)

    n_act = lax.fori_loop(0, n_local, listing, 0)

    def fetch(i):
        s, b = slots[i], lax.rem(i, NBUF)
        return [pltpu.make_async_copy(w1_hbm.at[s], b1.at[b], wsem.at[0, b]),
                pltpu.make_async_copy(w3_hbm.at[s], b3.at[b], wsem.at[1, b]),
                pltpu.make_async_copy(w2_hbm.at[s], b2.at[b], wsem.at[2, b])]

    def start(i):
        @pl.when(i < n_act)
        def _():
            for cp in fetch(i):
                cp.start()

    for i in range(NBUF):
        start(i)

    upper = (lax.broadcasted_iota(I32, (LANES, LANES), 0) < lax.broadcasted_iota(I32, (LANES, LANES), 1))
    upper = upper.astype(F32).astype(BF16)
    lane = lax.broadcasted_iota(I32, (NUM_EXPERTS, LANES), 1)
    code = lax.broadcasted_iota(I32, (NUM_EXPERTS, LANES), 0).astype(F32) + ONE
    run = jnp.zeros((NUM_EXPERTS, 1), F32)
    table = jnp.zeros((NUM_EXPERTS, LANES), F32)
    for j in range(n_blk):
        if j < PEERS:
            blk = wm_ref[j]
            w = jnp.zeros((NUM_EXPERTS, LANES), F32)
            for k in range(6):
                w += jnp.where(code == blk[k:k + 1, :], blk[PEERS + k:9 + k, :], ZERO)
        else:
            ids = jnp.concatenate([we_ref[2 * (j - PEERS)][:1, :EXT], we_ref[2 * (j - PEERS) + 1][:1, :EXT]], axis=1)
            w = jnp.where(code == ids, ONE, ZERO)
        mask = jnp.where(w != ZERO, ONE, ZERO)
        pos = dot(mask.astype(BF16), upper) + run
        run += jnp.sum(mask, axis=1, keepdims=True)
        table += jnp.where(lane == j + 1, run, ZERO)
        rank[j] = jnp.where(mask > ZERO, pos, -ONE)
        wrow[j] = w
    startv[...] = table.astype(I32)
    tc = pltpu.make_async_copy(startv, starts, xsem.at[2])
    tc.start()
    tc.wait()

    def list_units(i, n):
        e = experts[i]
        units = (starts[e, n_blk] + UNIT - 1) >> 7

        def put(u, n):
            ent_e[n] = e
            ent_u[n] = u
            ent_i[n] = i
            return n + 1
        return lax.fori_loop(0, units, put, n)

    n_all = lax.fori_loop(0, n_act, list_units, 0)
    for cp in xl:
        cp.wait()

    def out_copies(j):
        if j < PEERS:
            return pltpu.make_async_copy(pv.at[pl.ds(j * LANES, LANES)], pm_out.at[pl.ds(j * LANES, LANES)], osem.at[j])
        return pltpu.make_async_copy(pev.at[pl.ds((j - PEERS) * LANES, LANES)], pe_out.at[pl.ds((j - PEERS) * LANES, LANES)], osem.at[j])

    def finish(j):
        if j >= PEERS:
            pev[(j - PEERS) * LANES:(j - 7) * LANES, :] = pv[j * LANES:(j + 1) * LANES, :].astype(BF16)
        out_copies(j).start()

    def flush(first, n_ent, last):
        for j in range(n_blk):
            n_tiles[j] = 0

        def list_tiles(g, carry):
            e, u = ent_e[first + g], ent_u[first + g] * UNIT
            def span(blocks, hi):
                for j in blocks:
                    lo, hi = hi, jnp.clip(starts[e, j + 1] - u, 0, UNIT)
                    k0 = lo >> TILE_BITS
                    k1 = jnp.where(hi > lo, ((hi - 1) >> TILE_BITS) + 1, k0)
                    t = n_tiles[j]

                    def put(k, t, j=j):
                        tile_e[j * TILES + t] = e
                        tile_row[j * TILES + t] = g * UNIT + k * TILE
                        tile_rank[j * TILES + t] = u + k * TILE

                    put(k0, t)
                    put(k0 + 1, t + 1)
                    n_tiles[j] = t + k1 - k0

                    @pl.when(k1 > k0 + 2)
                    def _():
                        lax.fori_loop(2, k1 - k0, lambda k, _: put(k0 + k, t + k), None)

            span(range(PEERS), jnp.clip(-u, 0, UNIT))

            @pl.when(starts[e, n_blk] > starts[e, PEERS])
            def _():
                span(range(PEERS, n_blk), jnp.clip(starts[e, PEERS] - u, 0, UNIT))
            return carry

        lax.fori_loop(0, n_ent, list_tiles, 0)
        for j in range(n_blk):
            n_tile = n_tiles[j]

            def one_pass(p, carry, j=j, n_tile=n_tile):
                parts = []
                for g in range(GROUP):
                    t = p * GROUP + g
                    live = t < n_tile
                    e = jnp.where(live, tile_e[j * TILES + t], 0)
                    at = jnp.where(live, tile_row[j * TILES + t], 0)
                    base = jnp.where(live, tile_rank[j * TILES + t], -1000)
                    kb[g * TILE:(g + 1) * TILE, :] = obuf[pl.ds(pl.multiple_of(at, TILE), TILE), :]
                    rows = lax.broadcasted_iota(I32, (TILE, LANES), 0) + base
                    hit = rows.astype(F32) == rank[j, pl.ds(e, 1), :]
                    parts.append(jnp.where(hit, wrow[j, pl.ds(e, 1), :], ZERO))
                st = jnp.transpose(jnp.concatenate(parts, axis=0))
                res = dot(jnp.concatenate(split3(st), axis=0), kb[...])
                res = res[:LANES] + res[LANES:256] + res[256:]
                fresh = (first == 0) & (p == 0)

                @pl.when(fresh)
                def _():
                    pv[j * LANES:(j + 1) * LANES, :] = res

                @pl.when(jnp.logical_not(fresh))
                def _():
                    pv[j * LANES:(j + 1) * LANES, :] += res
                return carry

            @pl.when((first == 0) & (n_tile == 0))
            def _():
                pv[j * LANES:(j + 1) * LANES, :] = jnp.zeros((LANES, pv.shape[1]), F32)
            lax.fori_loop(0, (n_tile + GROUP - 1) >> CHIPS, one_pass, 0)

            @pl.when(last)
            def _():
                finish(j)

    def wait_for(k, carry):
        for cp in fetch(k):
            cp.wait()
        return carry

    def batch(bt, nxt):
        first = bt * MAXENT
        n_ent = jnp.minimum(n_all - first, MAXENT)

        def collect(q, carry):
            es = [jnp.minimum(q * TAKE + g, n_ent - 1) + first for g in range(TAKE)]
            ext = functools.reduce(jnp.logical_or, [starts[ent_e[n], n_blk] > starts[ent_e[n], PEERS] for n in es])

            def take(width):
                sel = []
                for n in es:
                    rows = (lax.broadcasted_iota(I32, (UNIT, LANES), 0) + ent_u[n] * UNIT).astype(F32)
                    e = ent_e[n]
                    sel.append(jnp.concatenate([jnp.where(rows == rank[j, pl.ds(e, 1), :], ONE, ZERO).astype(BF16)
                                                for j in range(width // LANES)], axis=1))
                got = dot(jnp.concatenate(sel, axis=0), xv[:width, :])
                obuf[pl.ds(pl.multiple_of(q * TAKE * UNIT, UNIT), TAKE * UNIT), :] = got.astype(BF16)

            @pl.when(ext)
            def _():
                take(n_tok)

            @pl.when(jnp.logical_not(ext))
            def _():
                take(n_main)
            return carry

        lax.fori_loop(0, (n_ent + TAKE - 1) // TAKE, collect, 0)

        def run_ffn(k, nxt):
            i = ent_i[first + k]

            def settle(k, carry):
                wait_for(k, carry)

                @pl.when(k < i)
                def _():
                    start(k + NBUF)
                return carry
            lax.fori_loop(nxt, i + 1, settle, 0)
            b = lax.rem(i, NBUF)
            two = (k + 1 < n_ent) & (ent_i[first + k + 1] == i)

            def ffn(n):
                rows = pl.ds(pl.multiple_of(k * UNIT, UNIT), n)
                xg = obuf[rows, :]
                act = (jax.nn.silu(dot(xg, b1[b])) * dot(xg, b3[b])).astype(BF16)
                obuf[rows, :] = dot(act, b2[b]).astype(BF16)

            @pl.when(two)
            def _():
                ffn(2 * UNIT)

            @pl.when(jnp.logical_not(two))
            def _():
                ffn(UNIT)
            end = k + jnp.where(two, 2, 1)

            @pl.when((first + end == n_all) | (ent_i[first + end] != i))
            def _():
                start(i + NBUF)
            return end, jnp.maximum(nxt, i + 1)

        nxt = lax.while_loop(lambda s: s[0] < n_ent, lambda s: run_ffn(*s), (0, nxt))[1]
        flush(first, n_ent, first + n_ent == n_all)
        return nxt

    nxt = lax.fori_loop(0, (n_all + MAXENT - 1) // MAXENT, batch, 0)

    def drain(k, carry):
        wait_for(k, carry)
        start(k + NBUF)
        return carry

    lax.fori_loop(nxt, n_act, drain, 0)

    @pl.when(n_all == 0)
    def _():
        pv[...] = jnp.zeros_like(pv)
        for j in range(n_blk):
            finish(j)
    for j in range(n_blk):
        out_copies(j).wait()


def scatter_kernel(pm_hbm, pe_hbm, z_ref, gw_ref, y_ref,
                   out_ref, mo, md, mrg, mrf, mrs, mfin, eo, ed, erg, erf, ers, gsib, ecr, ssem, rsem, lsem):
    me, c, h, sib, yn, zn, mir, first, second, diag = dims()
    cols = mo.shape[-1]
    mine = pl.ds(pl.multiple_of(c * cols, LANES), cols)
    theirs = pl.ds(pl.multiple_of((1 - c) * cols, LANES), cols)
    local, peer = [], []
    for base, (src, own, got, chips, swap) in ((0, (pe_hbm, eo, ed, (diag, yn, zn, me), (0, 1, 2, 3))),
                                               (CHIPS, (pm_hbm, mo, md, (diag, first, second, me), (0, 2, 1, 3)))):
        for i in range(CHIPS):
            rows = pl.ds(2 * ((chips[i] % PEERS) // 2), 2)
            sib_rows = pl.ds(2 * ((chips[swap[i]] % PEERS) // 2), 2)
            local.append(pltpu.make_async_copy(src.at[rows, :, mine], own.at[i], lsem.at[base + i]))
            peer.append(pltpu.make_async_remote_copy(
                src_ref=src.at[sib_rows, :, theirs], dst_ref=got.at[i], send_sem=ssem.at[base + i],
                recv_sem=rsem.at[base + i], device_id={"ep": sib}, device_id_type=MESH))
    for i in (0, CHIPS, 1, 5, 2, 6, 3, 7):
        local[i].start()
    barrier([{"ep": sib}, {"ep": yn}, {"ep": zn}, {"ep": mir}])
    for i in (0, CHIPS, 1, 5, 2, 6, 3, 7):
        peer[i].start()

    def rcopy(src, dst, i, dev):
        return pltpu.make_async_remote_copy(src_ref=src, dst_ref=dst, send_sem=ssem.at[i], recv_sem=rsem.at[i],
                                            device_id={"ep": dev}, device_id_type=MESH)

    eg, ef, es = rcopy(eo.at[0], erg, PEERS, yn), rcopy(eo.at[1], erf, 9, yn), rcopy(eo.at[2], ers, 10, zn)
    back = rcopy(eo.at[3], ecr, 11, mir)
    gshare = rcopy(gw_ref, gsib, 12, sib)
    order = (1 - c, c)
    mg = [rcopy(mo.at[0, b], mrg.at[b], 13 + n, first) for n, b in enumerate(order)]
    ms = [rcopy(mo.at[2, b], mrs.at[b], 15 + n, second) for n, b in enumerate(order)]
    mf = rcopy(mo.at[1], mrf, 17, first)
    mfinal = rcopy(mo.at[3, 1 - c], mfin, 18, sib)

    def joined(own, got, i, base):
        local[base + i].wait()
        peer[base + i].wait_recv()
        own[i] = own[i] + got[i]

    joined(eo, ed, 0, 0)
    eg.start()
    joined(mo, md, 0, CHIPS)
    mg[0].start()
    joined(eo, ed, 1, 0)
    ef.start()
    mg[1].start()
    joined(eo, ed, 2, 0)
    joined(eo, ed, 3, 0)
    gshare.start()
    eg.wait_recv()
    eo[2] = eo[2] + erg[...]
    es.start()
    joined(mo, md, 1, CHIPS)
    mf.start()
    joined(mo, md, 2, CHIPS)
    mg[0].wait_recv()
    mo[2, 1 - c] = mo[2, 1 - c] + mrg[1 - c]
    ms[0].start()
    ef.wait_recv()
    es.wait_recv()
    eo[3] = eo[3] + erf[...] + ers[...]
    back.start()
    joined(mo, md, 3, CHIPS)
    out_ref[...] = z_ref[...]
    mg[1].wait_recv()
    mo[2, c] = mo[2, c] + mrg[c]
    ms[1].start()
    mf.wait_recv()
    mo[3] = mo[3] + mrf[...]
    gshare.wait_recv()
    back.wait_recv()
    for b, g in ((c, gw_ref), (1 - c, gsib)):
        for part in split3(g[...]):
            mo[3, b] += dot(part, ecr[b], 0, 0)
    ms[0].wait_recv()
    mo[3, 1 - c] = mo[3, 1 - c] + mrs[1 - c]
    mfinal.start()
    ms[1].wait_recv()
    out_ref[:, mine] += mo[3, c] + mrs[c]
    mfinal.wait_recv()
    out_ref[:, theirs] += mfin[...]
    y_ref[...] = out_ref[...].astype(y_ref.dtype)
    for cp in peer + mg + ms + [eg, ef, es, back, gshare, mf, mfinal]:
        cp.wait_send()


def solution(mesh):
    any_space = pl.BlockSpec(memory_space=pl.ANY)
    vmem = pl.BlockSpec(memory_space=pltpu.VMEM)
    smem = pl.BlockSpec(memory_space=pltpu.SMEM)
    sds = jax.ShapeDtypeStruct

    def gather(x, at, se, rnd, wr, w1, w3, w2):
        d, ff = w1.shape
        return pl.pallas_call(
            gather_kernel,
            out_shape=(sds((PEERS, LANES, d), BF16), sds((PEERS, EXT, d), BF16), sds((PEERS, 16, LANES), F32),
                       sds((PEERS, PEERS, LANES), F32), sds((PEERS, LANES), I32), sds((EXT, LANES), F32),
                       sds((LANES, d), F32), sds((1, 1), I32)),
            in_specs=[vmem, vmem, vmem, smem, vmem] + [any_space] * 3,
            out_specs=(any_space,) * CHIPS + (vmem,) * CHIPS,
            scratch_shapes=[
                pltpu.VMEM((PEERS, LANES, d), BF16), pltpu.VMEM((PEERS, EXT, d), BF16),
                pltpu.VMEM((PEERS, 16, LANES), F32), pltpu.VMEM((PEERS, PEERS, LANES), F32),
                pltpu.VMEM((EXT, d), BF16), pltpu.VMEM((PEERS, LANES), F32),
                pltpu.VMEM((EXT, d), BF16), pltpu.VMEM((PEERS, LANES), F32), pltpu.VMEM((16, LANES), F32),
                pltpu.VMEM((2, NUM_EXPERTS, LANES), F32), pltpu.VMEM((NUM_EXPERTS, LANES), F32),
                pltpu.VMEM((5, PEERS, LANES), F32), pltpu.VMEM((5, PEERS, LANES), F32),
                pltpu.VMEM((d, ff), BF16), pltpu.VMEM((d, ff), BF16), pltpu.VMEM((ff, d), BF16),
                pltpu.SemaphoreType.DMA((60,)), pltpu.SemaphoreType.DMA((60,)), pltpu.SemaphoreType.DMA((21,)),
            ],
            compiler_params=pltpu.CompilerParams(collective_id=0, has_side_effects=True),
            name="gather_rows",
        )(x, at, se, rnd, wr, w1, w3, w2)

    def experts(own, se, xm, xe, wm, we, w1, w3, w2):
        _, d, ff = w1.shape
        n_tok = PEERS * (LANES + EXT)
        return pl.pallas_call(
            expert_kernel,
            out_shape=(sds((PEERS * LANES, d), F32), sds((PEERS * EXT, d), BF16)),
            in_specs=[smem, smem, any_space, any_space, vmem, vmem] + [any_space] * 3,
            out_specs=(any_space, any_space),
            scratch_shapes=[
                pltpu.VMEM((n_tok, d), BF16), pltpu.VMEM((n_tok // LANES, NUM_EXPERTS, LANES), F32), pltpu.VMEM((n_tok // LANES, NUM_EXPERTS, LANES), F32),
                pltpu.VMEM((n_tok, d), F32), pltpu.VMEM((PEERS * EXT, d), BF16), pltpu.VMEM((MAXENT * UNIT, d), BF16),
                pltpu.VMEM((GROUP * TILE, d), BF16),
                pltpu.VMEM((NUM_EXPERTS, LANES), I32), pltpu.SMEM((NUM_EXPERTS, LANES), I32),
                pltpu.VMEM((NBUF, d, ff), BF16), pltpu.VMEM((NBUF, d, ff), BF16), pltpu.VMEM((NBUF, ff, d), BF16),
                pltpu.SMEM((32,), I32), pltpu.SMEM((32,), I32), pltpu.SMEM((NUM_EXPERTS,), I32),
                pltpu.SMEM((384,), I32), pltpu.SMEM((384,), I32), pltpu.SMEM((384,), I32),
                pltpu.SMEM((12 * TILES,), I32), pltpu.SMEM((12 * TILES,), I32), pltpu.SMEM((12 * TILES,), I32),
                pltpu.SMEM((16,), I32),
                pltpu.SemaphoreType.DMA((3, NBUF)), pltpu.SemaphoreType.DMA((3,)), pltpu.SemaphoreType.DMA((12,)),
            ],
            name="expert_rows",
        )(own, se, xm, xe, wm, we, w1, w3, w2)

    def scatter(pm, pe, z, gw, last):
        d = z.shape[1]
        half = d // 2
        big, small = (2, LANES, half), (2, EXT, half)
        return pl.pallas_call(
            scatter_kernel,
            out_shape=sds((LANES, d), F32),
            in_specs=[any_space, any_space, vmem, vmem],
            out_specs=vmem,
            scratch_shapes=[
                pltpu.VMEM((LANES, d), F32),
                pltpu.VMEM((CHIPS,) + big, F32), pltpu.VMEM((CHIPS,) + big, F32),
                pltpu.VMEM(big, F32), pltpu.VMEM(big, F32), pltpu.VMEM(big, F32), pltpu.VMEM((LANES, half), F32),
                pltpu.VMEM((CHIPS,) + small, BF16), pltpu.VMEM((CHIPS,) + small, BF16),
                pltpu.VMEM(small, BF16), pltpu.VMEM(small, BF16), pltpu.VMEM(small, BF16), pltpu.VMEM((EXT, LANES), F32),
                pltpu.VMEM(small, BF16),
                pltpu.SemaphoreType.DMA((20,)), pltpu.SemaphoreType.DMA((20,)), pltpu.SemaphoreType.DMA((PEERS,)),
            ],
            compiler_params=pltpu.CompilerParams(collective_id=1 if last else 2, has_side_effects=True),
            name="scatter_sums" if last else "scatter_more",
        )(pm, pe, z, gw)

    def device_step(x, slot_expert, w1, w3, w2, assign, wr, w1s, w3s, w2s):
        d = x.shape[1]
        rows_of = lambda a: a.reshape(-1, d)

        def gathered(r):
            return gather(x, assign.T, slot_expert, r.reshape(1), wr.T, w1s, w3s, w2s)

        def summed(parts):
            xm, xe, wm, we, own = parts
            pm, pe = experts(own, slot_expert, rows_of(xm), rows_of(xe), wm, we, w1, w3, w2)
            return pm.reshape(PEERS, LANES, d), pe.reshape(PEERS, EXT, d)

        def again(carry):
            r, n, z = carry
            *parts, gw, _, _ = gathered(r)
            return r + 1, n, scatter(*summed(parts), z, gw, False)

        *parts, gw, z, nr = gathered(jnp.int32(0))
        z = lax.while_loop(lambda s: s[0] < s[1], again, (jnp.int32(1), nr.reshape(()), z))[2]
        return scatter(*summed(parts), z, gw, True).astype(BF16)

    tok = P(("dp", "ep"), None)
    slot = P("ep", None, None)
    return jax.shard_map(device_step, mesh=mesh,
                         in_specs=(tok, P(), slot, slot, slot, tok, P(), P(), P(), P()),
                         out_specs=tok, check_vma=False)
```

```python
import functools

import jax
import jax.numpy as jnp
from jax import lax
from jax.experimental import pallas as pl
from jax.experimental.pallas import tpu as pltpu
from jax.sharding import PartitionSpec as P

ROUTE_SCALE = 2.5
LANES, PEERS, CHIPS = 128, 8, 4
ZERO, ONE = 0.0, 1.0
MESH = pl.DeviceIdType.MESH
NUM_EXPERTS = 64
EXT = 64
UNIT = LANES
PIECES = 2
NBUF = 6
MAXENT = 15
GROUP = 16
FEW = 4
TILES = 160
TILE_BITS = CHIPS
TILE = 1 << TILE_BITS
TAKE = 3
F32, BF16, I32 = jnp.float32, jnp.bfloat16, jnp.int32


def dims():
    me = lax.axis_index("ep")
    c, y, z, h = me % 2, (me // 2) % 2, (me // CHIPS) % 2, me // PEERS
    sib = me + 1 - 2 * c
    yn = me + 2 - CHIPS * y
    zn = me + CHIPS - PEERS * z
    mir = me + PEERS - 16 * h
    first = yn + c * (zn - yn)
    second = zn + c * (yn - zn)
    diag = yn + zn - me
    return me, c, h, sib, yn, zn, mir, first, second, diag


def barrier(peers):
    sem = pltpu.get_barrier_semaphore()
    for peer in peers:
        pl.semaphore_signal(sem, inc=1, device_id=peer, device_id_type=MESH)
    pl.semaphore_wait(sem, len(peers))


def dot(a, b, ca=1, cb=0):
    return lax.dot_general(a, b, (((ca,), (cb,)), ((), ())), preferred_element_type=F32)


def split3(v):
    hi = v.astype(BF16)
    rest = v - hi.astype(F32)
    mid = rest.astype(BF16)
    lo = (rest - mid.astype(F32)).astype(BF16)
    return hi, mid, lo


def gather_kernel(x_ref, at_ref, se_ref, rnd_ref, wr_ref, w1_hbm, w3_hbm, w2_hbm,
                  xm_out, xe_out, wm_out, we_out, own_out, gw_out, z_out, nr_out,
                  xs, xes, wms, wes, xcr, ecr, xsnd, esnd, wsnd, cand_s, own_s, flag_s, frecv,
                  w1s, w3s, w2s, ssem, rsem, lsem):
    me, c, h, sib, yn, zn, mir, first, second, diag = dims()
    dp = lax.axis_index("dp")
    qm, qf, qs, qg = me % PEERS, first % PEERS, second % PEERS, diag % PEERS
    loads = [pltpu.make_async_copy(a, b, lsem.at[i]) for i, (a, b) in
             enumerate(((w1_hbm, w1s), (w3_hbm, w3s), (w2_hbm, w2s)))]
    for cp in loads:
        cp.start()
    barrier([{"ep": sib}, {"ep": yn}, {"ep": zn}, {"ep": mir}, {"dp": 1 - dp}])

    def rcopy(src, dst, i, dev):
        return pltpu.make_async_remote_copy(src_ref=src, dst_ref=dst, send_sem=ssem.at[i], recv_sem=rsem.at[i],
                                            device_id=dev, device_id_type=MESH)

    def spread(own, buf, base, one, two):
        ep = lambda d: {"ep": d}
        q1, q2 = one % PEERS, two % PEERS
        return [rcopy(own, buf.at[qm], base, ep(one)), rcopy(own, buf.at[qm], base + 1, ep(two)),
                rcopy(own, buf.at[qm], base + 2, ep(sib)), rcopy(buf.at[q1], buf.at[q1], base + 3, ep(two)),
                rcopy(buf.at[q1], buf.at[q1], base + CHIPS, ep(sib)), rcopy(buf.at[q2], buf.at[q2], base + 5, ep(sib)),
                rcopy(buf.at[qg], buf.at[qg], base + 6, ep(sib))]

    parts = [pl.ds(i * (x_ref.shape[0] // PIECES), x_ref.shape[0] // PIECES) for i in range(PIECES)]
    ax = [spread(x_ref.at[r], xs.at[:, r], 45 + 7 * i, first, second) for i, r in enumerate(parts)]
    for i in range(2):
        ax[0][i].start()

    n_tok = x_ref.shape[0]
    n_slots = se_ref.shape[0]
    rnd = jnp.full((1, 1), rnd_ref[0], I32).astype(F32)
    first_round = jnp.where(rnd == ZERO, ONE, ZERO)
    expert_of = se_ref[...].reshape(1, n_slots)
    eye = (lax.broadcasted_iota(I32, (NUM_EXPERTS, n_slots), 0) == expert_of).astype(F32)
    eye_bf = eye.astype(BF16)
    lane_slot = lax.broadcasted_iota(I32, (1, n_slots), 1)
    per_half = n_slots // 2
    here = jnp.where((lane_slot >= h * per_half) & (lane_slot < (h + 1) * per_half), ONE, ZERO)
    avail = jnp.where(jnp.sum(eye * here, axis=1, keepdims=True) > ZERO, ONE, ZERO)
    row_slot = lax.broadcasted_iota(I32, (n_slots, n_tok), 0)
    hot = jnp.concatenate([(row_slot == at_ref[k:k + 1, :]).astype(F32).astype(BF16) for k in range(6)], axis=1)
    picks_all = dot(eye_bf, hot)
    picks = [picks_all[:, k * n_tok:(k + 1) * n_tok] for k in range(6)]
    code = lax.broadcasted_iota(I32, (NUM_EXPERTS, n_tok), 0).astype(F32) + ONE
    ids = [jnp.sum(p * code, axis=0, keepdims=True) for p in picks]
    miss = [jnp.sum(p * (ONE - avail), axis=0, keepdims=True) for p in picks]
    none = jnp.zeros((2, n_tok), F32)
    id_all = jnp.concatenate(ids + [none], axis=0)
    miss_all = jnp.concatenate(miss + [none], axis=0)

    upper = (lax.broadcasted_iota(I32, (n_tok, n_tok), 0) < lax.broadcasted_iota(I32, (n_tok, n_tok), 1))
    before = dot(miss_all.astype(BF16), upper.astype(F32).astype(BF16))
    offset = -EXT * rnd
    count = jnp.zeros((1, 1), F32)
    row_ext = lax.broadcasted_iota(I32, (EXT, n_tok), 0).astype(F32)
    sels = []
    for k in range(6):
        sels.append(jnp.where((row_ext == before[k:k + 1, :] + offset) & (miss[k] > ZERO), ONE, ZERO))
        mk = jnp.sum(miss[k], axis=1, keepdims=True)
        offset += mk
        count += mk
    take = functools.reduce(lambda a, b: a + b, sels)
    xsnd[...] = dot(take.astype(BF16), x_ref[...]).astype(BF16)
    piece = [pl.ds(i * (EXT // PIECES), EXT // PIECES) for i in range(PIECES)]
    cross = [rcopy(xsnd.at[r], xcr.at[r], 20 + i, {"ep": mir}) for i, r in enumerate(piece)]
    cross.append(rcopy(esnd, ecr, 19, {"ep": mir}))
    for cp in cross[:-1]:
        cp.start()
    codes = jnp.zeros((PEERS, EXT), F32)
    for k in range(6):
        codes += dot(jnp.broadcast_to(ids[k], (PEERS, n_tok)).astype(BF16), sels[k].astype(BF16), 1, 1)
    esnd[...] = jnp.concatenate([codes, jnp.zeros((PEERS, LANES - EXT), F32)], axis=1)
    cross[-1].start()
    for a in ax[1:]:
        for i in range(2):
            a[i].start()
    for a in ax:
        a[2].start()

    gate = jax.nn.sigmoid(dot(wr_ref[...], x_ref[...], 1, 1))
    picked = gate * functools.reduce(lambda a, b: a + b, picks)
    total = jnp.sum(picked, axis=0, keepdims=True)
    weight = ROUTE_SCALE * picked / jnp.maximum(total, 1e-30)
    wk = [jnp.sum(p * weight, axis=0, keepdims=True) for p in picks]
    w_all = jnp.concatenate(wk + [none], axis=0) * (ONE - miss_all) * first_round
    packed = jnp.concatenate([id_all, w_all], axis=0)
    wsnd[...] = packed
    wms[qm] = packed
    aw = spread(wsnd, wms, 7, first, second)
    for i in range(3):
        aw[i].start()
    gw_out[...] = functools.reduce(lambda a, b: a + b, [sel * w for sel, w in zip(sels, wk)])
    flag_s[0] = jnp.broadcast_to(jnp.floor((count + (EXT - 1)) * (ONE / EXT)), (PEERS, LANES))
    steps = [rcopy(flag_s.at[i], frecv.at[i], 14 + i, d) for i, d in
             enumerate(({"dp": 1 - dp}, {"ep": sib}, {"ep": mir}, {"ep": zn}, {"ep": yn}))]
    steps[0].start()

    def vote(i):
        steps[i].wait()
        flag_s[i + 1] = jnp.maximum(flag_s[i], frecv[i])
        steps[i + 1].start()

    outs = []

    def put_out(src, dst, i):
        outs.append(pltpu.make_async_copy(src, dst, lsem.at[i]))
        outs[-1].start()

    put_out(x_ref, xm_out.at[qm], 3)

    slot_row = lax.broadcasted_iota(I32, (n_slots, LANES), 0)
    lane_dev = lax.broadcasted_iota(I32, (n_slots, LANES), 1)
    lo = (lane_dev + PEERS * h) * (n_slots // 16)
    block = ((slot_row >= lo) & (slot_row < lo + n_slots // 16) & (lane_dev < PEERS)).astype(F32).astype(BF16)
    cand = jnp.where(dot(eye_bf, block) > ZERO, ONE, ZERO)
    several = jnp.where(jnp.sum(cand, axis=1, keepdims=True) > ONE, ONE, ZERO)
    lane = lax.broadcasted_iota(I32, (1, LANES), 1).astype(F32)
    block_key = jnp.where(cand > ZERO, jnp.broadcast_to(lane, cand.shape), 1e9)
    cand_s[0] = block_key
    there = jnp.where(jnp.sum(eye * (ONE - here), axis=1, keepdims=True) > ZERO, 2.0, 5.0)
    cand_s[1] = jnp.broadcast_to(several * there, cand.shape)
    load0 = jnp.sum(cand * (ONE - several) * there, axis=0, keepdims=True)

    def pick(e, load):
        key = cand_s[0, pl.ds(e, 1), :] + load * 256.0
        best = jnp.min(key, axis=1, keepdims=True)
        sel = jnp.where((key == best) & (key < 1e8), ONE, ZERO)
        own_s[pl.ds(e, 1), :] = sel
        return load + sel * cand_s[1, pl.ds(e, 1), :]

    load1 = lax.fori_loop(0, NUM_EXPERTS // 2, pick, load0)
    vote(0)

    for a in ax + [aw]:
        a[0].wait_recv()
        a[3].start()
        a[CHIPS].start()
    for a in ax + [aw]:
        a[1].wait_recv()
        a[5].start()
    put_out(xs.at[qf], xm_out.at[qf], CHIPS)
    put_out(xs.at[qs], xm_out.at[qs], 5)
    vote(1)
    lax.fori_loop(NUM_EXPERTS // 2, NUM_EXPERTS, pick, load1)
    mine = jnp.where(lax.broadcasted_iota(I32, (PEERS, LANES), 1) == qm, ONE, ZERO)
    own = dot(mine.astype(BF16), own_s[...].astype(BF16), 1, 1)
    own_out[...] = jnp.concatenate([own, jnp.zeros((PEERS, LANES - NUM_EXPERTS), F32)], axis=1).astype(I32)
    vote(2)

    ew = spread(ecr, wes, 24, zn, yn)
    ex = [spread(xcr.at[r], xes.at[:, r], 31 + 7 * i, zn, yn) for i, r in enumerate(piece)]
    for i, a in enumerate(ex):
        cross[i].wait_recv()
        for n in range(3):
            a[n].start()
    cross[-1].wait_recv()
    wes[qm] = ecr[...]
    for n in range(3):
        ew[n].start()
    put_out(xcr, xe_out.at[qm], 6)
    vote(3)

    for cp in loads:
        cp.wait()
    hg = dot(x_ref[...], w1s[...])
    hu = dot(x_ref[...], w3s[...])
    act = (jax.nn.silu(hg) * hu).astype(BF16)
    z_out[...] = dot(act, w2s[...]) * first_round

    for a in ex + [ew]:
        a[0].wait_recv()
        a[3].start()
        a[CHIPS].start()
    for a in ex + [ew]:
        a[1].wait_recv()
        a[5].start()
    put_out(xes.at[zn % PEERS], xe_out.at[zn % PEERS], 7)
    put_out(xes.at[yn % PEERS], xe_out.at[yn % PEERS], PEERS)
    for a in ax + [aw]:
        a[3].wait_recv()
        a[6].start()
    put_out(xs.at[qg], xm_out.at[qg], 9)
    for n, i in enumerate((2, CHIPS, 5, 6)):
        for a in ax + [aw]:
            a[i].wait_recv()
        q = (sib % PEERS, qs + 1 - 2 * c, qf + 1 - 2 * c, qg + 1 - 2 * c)[n]
        put_out(xs.at[q], xm_out.at[q], 10 + n)
    steps[CHIPS].wait()
    nr_out[...] = jnp.maximum(flag_s[CHIPS], frecv[CHIPS])[0:1, 0:1].astype(I32)
    for a in ex + [ew]:
        a[3].wait_recv()
        a[6].start()
    put_out(xes.at[qg], xe_out.at[qg], 14)
    for n, i in enumerate((2, CHIPS, 5, 6)):
        for a in ex + [ew]:
            a[i].wait_recv()
        q = (sib % PEERS, zn % PEERS + 1 - 2 * c, yn % PEERS + 1 - 2 * c, qg + 1 - 2 * c)[n]
        put_out(xes.at[q], xe_out.at[q], 15 + n)
    put_out(wms, wm_out, 19)
    put_out(wes, we_out, 20)
    for a in [aw, ew, cross] + ax + ex:
        for cp in a:
            cp.wait_send()
    for cp in outs:
        cp.wait()


def expert_kernel(own_ref, se_ref, xm_hbm, xe_hbm, wm_ref, we_ref, w1_hbm, w3_hbm, w2_hbm, pm_out, pe_out,
                  xv, wrow, rank, pv, pev, obuf, kb, startv, starts, b1, b3, b2, slots, experts, seen, ent_e, ent_u, ent_i,
                  tile_e, tile_row, tile_rank, n_tiles, wsem, xsem, osem):
    me = lax.axis_index("ep")
    n_local = w1_hbm.shape[0]
    n_main, n_ext = PEERS * LANES, PEERS * EXT
    n_tok = n_main + n_ext
    n_blk = n_tok // LANES
    xl = [pltpu.make_async_copy(xm_hbm, xv.at[pl.ds(0, n_main)], xsem.at[0]),
          pltpu.make_async_copy(xe_hbm, xv.at[pl.ds(n_main, n_ext)], xsem.at[1])]
    for cp in xl:
        cp.start()

    def clear(e, carry):
        seen[e] = 0
        return carry

    lax.fori_loop(0, NUM_EXPERTS, clear, 0)

    def listing(s, n):
        e = se_ref[me * n_local + s]
        use = (own_ref[0, e] == 1) & (seen[e] == 0)

        @pl.when(use)
        def _():
            slots[n] = s
            experts[n] = e
            seen[e] = 1
        return jnp.where(use, n + 1, n)

    n_act = lax.fori_loop(0, n_local, listing, 0)

    def fetch(i):
        s, b = slots[i], lax.rem(i, NBUF)
        return [pltpu.make_async_copy(w1_hbm.at[s], b1.at[b], wsem.at[0, b]),
                pltpu.make_async_copy(w3_hbm.at[s], b3.at[b], wsem.at[1, b]),
                pltpu.make_async_copy(w2_hbm.at[s], b2.at[b], wsem.at[2, b])]

    def start(i):
        @pl.when(i < n_act)
        def _():
            for cp in fetch(i):
                cp.start()

    for i in range(NBUF):
        start(i)

    upper = (lax.broadcasted_iota(I32, (LANES, LANES), 0) < lax.broadcasted_iota(I32, (LANES, LANES), 1))
    upper = upper.astype(F32).astype(BF16)
    lane = lax.broadcasted_iota(I32, (NUM_EXPERTS, LANES), 1)
    code = lax.broadcasted_iota(I32, (NUM_EXPERTS, LANES), 0).astype(F32) + ONE
    run = jnp.zeros((NUM_EXPERTS, 1), F32)
    table = jnp.zeros((NUM_EXPERTS, LANES), F32)
    for j in range(n_blk):
        if j < PEERS:
            blk = wm_ref[j]
            w = jnp.zeros((NUM_EXPERTS, LANES), F32)
            for k in range(6):
                w += jnp.where(code == blk[k:k + 1, :], blk[PEERS + k:9 + k, :], ZERO)
        else:
            ids = jnp.concatenate([we_ref[2 * (j - PEERS)][:1, :EXT], we_ref[2 * (j - PEERS) + 1][:1, :EXT]], axis=1)
            w = jnp.where(code == ids, ONE, ZERO)
        mask = jnp.where(w != ZERO, ONE, ZERO)
        pos = dot(mask.astype(BF16), upper) + run
        run += jnp.sum(mask, axis=1, keepdims=True)
        table += jnp.where(lane == j + 1, run, ZERO)
        rank[j] = jnp.where(mask > ZERO, pos, -ONE)
        wrow[j] = w
    startv[...] = table.astype(I32)
    tc = pltpu.make_async_copy(startv, starts, xsem.at[2])
    tc.start()
    tc.wait()

    def list_units(i, n):
        e = experts[i]
        units = (starts[e, n_blk] + UNIT - 1) >> 7

        def put(u, n):
            ent_e[n] = e
            ent_u[n] = u
            ent_i[n] = i
            return n + 1
        return lax.fori_loop(0, units, put, n)

    n_all = lax.fori_loop(0, n_act, list_units, 0)
    for cp in xl:
        cp.wait()

    def out_copies(j):
        if j < PEERS:
            return pltpu.make_async_copy(pv.at[pl.ds(j * LANES, LANES)], pm_out.at[pl.ds(j * LANES, LANES)], osem.at[j])
        return pltpu.make_async_copy(pev.at[pl.ds((j - PEERS) * LANES, LANES)], pe_out.at[pl.ds((j - PEERS) * LANES, LANES)], osem.at[j])

    def finish(j):
        if j >= PEERS:
            pev[(j - PEERS) * LANES:(j - 7) * LANES, :] = pv[j * LANES:(j + 1) * LANES, :].astype(BF16)
        out_copies(j).start()

    def flush(first, n_ent, last):
        for j in range(n_blk):
            n_tiles[j] = 0

        def list_tiles(g, carry):
            e, u = ent_e[first + g], ent_u[first + g] * UNIT
            def span(blocks, hi):
                for j in blocks:
                    lo, hi = hi, jnp.clip(starts[e, j + 1] - u, 0, UNIT)
                    k0 = lo >> TILE_BITS
                    k1 = jnp.where(hi > lo, ((hi - 1) >> TILE_BITS) + 1, k0)
                    t = n_tiles[j]

                    def put(k, t, j=j):
                        tile_e[j * TILES + t] = e
                        tile_row[j * TILES + t] = g * UNIT + k * TILE
                        tile_rank[j * TILES + t] = u + k * TILE

                    put(k0, t)
                    put(k0 + 1, t + 1)
                    n_tiles[j] = t + k1 - k0

                    @pl.when(k1 > k0 + 2)
                    def _():
                        lax.fori_loop(2, k1 - k0, lambda k, _: put(k0 + k, t + k), None)

            span(range(PEERS), jnp.clip(-u, 0, UNIT))

            @pl.when(starts[e, n_blk] > starts[e, PEERS])
            def _():
                span(range(PEERS, n_blk), jnp.clip(starts[e, PEERS] - u, 0, UNIT))
            return carry

        lax.fori_loop(0, n_ent, list_tiles, 0)
        for j in range(n_blk):
            n_tile = n_tiles[j]

            joint = GROUP if j < PEERS else FEW

            def one_pass(p, carry, j=j, n_tile=n_tile, joint=joint):
                parts = []
                for g in range(joint):
                    t = p * joint + g
                    live = t < n_tile
                    e = jnp.where(live, tile_e[j * TILES + t], 0)
                    at = jnp.where(live, tile_row[j * TILES + t], 0)
                    base = jnp.where(live, tile_rank[j * TILES + t], -1000)
                    kb[g * TILE:(g + 1) * TILE, :] = obuf[pl.ds(pl.multiple_of(at, TILE), TILE), :]
                    rows = lax.broadcasted_iota(I32, (TILE, LANES), 0) + base
                    hit = rows.astype(F32) == rank[j, pl.ds(e, 1), :]
                    parts.append(jnp.where(hit, wrow[j, pl.ds(e, 1), :], ZERO))
                st = jnp.transpose(jnp.concatenate(parts, axis=0))
                res = dot(jnp.concatenate(split3(st), axis=0), kb[:joint * TILE, :])
                res = res[:LANES] + res[LANES:256] + res[256:]
                fresh = (first == 0) & (p == 0)

                @pl.when(fresh)
                def _():
                    pv[j * LANES:(j + 1) * LANES, :] = res

                @pl.when(jnp.logical_not(fresh))
                def _():
                    pv[j * LANES:(j + 1) * LANES, :] += res
                return carry

            @pl.when((first == 0) & (n_tile == 0))
            def _():
                pv[j * LANES:(j + 1) * LANES, :] = jnp.zeros((LANES, pv.shape[1]), F32)
            lax.fori_loop(0, (n_tile + joint - 1) // joint, one_pass, 0)

            @pl.when(last)
            def _():
                finish(j)

    def wait_for(k, carry):
        for cp in fetch(k):
            cp.wait()
        return carry

    def batch(bt, nxt):
        first = bt * MAXENT
        n_ent = jnp.minimum(n_all - first, MAXENT)

        def collect(q, carry):
            es = [jnp.minimum(q * TAKE + g, n_ent - 1) + first for g in range(TAKE)]
            ext = functools.reduce(jnp.logical_or, [starts[ent_e[n], n_blk] > starts[ent_e[n], PEERS] for n in es])

            def take(width):
                sel = []
                for n in es:
                    rows = (lax.broadcasted_iota(I32, (UNIT, LANES), 0) + ent_u[n] * UNIT).astype(F32)
                    e = ent_e[n]
                    sel.append(jnp.concatenate([jnp.where(rows == rank[j, pl.ds(e, 1), :], ONE, ZERO).astype(BF16)
                                                for j in range(width // LANES)], axis=1))
                got = dot(jnp.concatenate(sel, axis=0), xv[:width, :])
                obuf[pl.ds(pl.multiple_of(q * TAKE * UNIT, UNIT), TAKE * UNIT), :] = got.astype(BF16)

            @pl.when(ext)
            def _():
                take(n_tok)

            @pl.when(jnp.logical_not(ext))
            def _():
                take(n_main)
            return carry

        lax.fori_loop(0, (n_ent + TAKE - 1) // TAKE, collect, 0)

        def run_ffn(k, nxt):
            i = ent_i[first + k]

            def settle(k, carry):
                wait_for(k, carry)

                @pl.when(k < i)
                def _():
                    start(k + NBUF)
                return carry
            lax.fori_loop(nxt, i + 1, settle, 0)
            b = lax.rem(i, NBUF)
            two = (k + 1 < n_ent) & (ent_i[first + k + 1] == i)

            def ffn(n):
                rows = pl.ds(pl.multiple_of(k * UNIT, UNIT), n)
                xg = obuf[rows, :]
                act = (jax.nn.silu(dot(xg, b1[b])) * dot(xg, b3[b])).astype(BF16)
                obuf[rows, :] = dot(act, b2[b]).astype(BF16)

            @pl.when(two)
            def _():
                ffn(2 * UNIT)

            @pl.when(jnp.logical_not(two))
            def _():
                ffn(UNIT)
            end = k + jnp.where(two, 2, 1)

            @pl.when((first + end == n_all) | (ent_i[first + end] != i))
            def _():
                start(i + NBUF)
            return end, jnp.maximum(nxt, i + 1)

        nxt = lax.while_loop(lambda s: s[0] < n_ent, lambda s: run_ffn(*s), (0, nxt))[1]
        flush(first, n_ent, first + n_ent == n_all)
        return nxt

    nxt = lax.fori_loop(0, (n_all + MAXENT - 1) // MAXENT, batch, 0)

    def drain(k, carry):
        wait_for(k, carry)
        start(k + NBUF)
        return carry

    lax.fori_loop(nxt, n_act, drain, 0)

    @pl.when(n_all == 0)
    def _():
        pv[...] = jnp.zeros_like(pv)
        for j in range(n_blk):
            finish(j)
    for j in range(n_blk):
        out_copies(j).wait()


def scatter_kernel(pm_hbm, pe_hbm, z_ref, gw_ref, y_ref,
                   out_ref, mo, md, mrg, mrf, mrs, mfin, eo, ed, erg, erf, ers, gsib, ecr, ssem, rsem, lsem):
    me, c, h, sib, yn, zn, mir, first, second, diag = dims()
    cols = mo.shape[-1]
    mine = pl.ds(pl.multiple_of(c * cols, LANES), cols)
    theirs = pl.ds(pl.multiple_of((1 - c) * cols, LANES), cols)
    local, peer = [], []
    for base, (src, own, got, chips, swap) in ((0, (pe_hbm, eo, ed, (diag, yn, zn, me), (0, 1, 2, 3))),
                                               (CHIPS, (pm_hbm, mo, md, (diag, first, second, me), (0, 2, 1, 3)))):
        for i in range(CHIPS):
            rows = pl.ds(2 * ((chips[i] % PEERS) // 2), 2)
            sib_rows = pl.ds(2 * ((chips[swap[i]] % PEERS) // 2), 2)
            local.append(pltpu.make_async_copy(src.at[rows, :, mine], own.at[i], lsem.at[base + i]))
            peer.append(pltpu.make_async_remote_copy(
                src_ref=src.at[sib_rows, :, theirs], dst_ref=got.at[i], send_sem=ssem.at[base + i],
                recv_sem=rsem.at[base + i], device_id={"ep": sib}, device_id_type=MESH))
    for i in (0, CHIPS, 1, 5, 2, 6, 3, 7):
        local[i].start()
    barrier([{"ep": sib}, {"ep": yn}, {"ep": zn}, {"ep": mir}])
    for i in (0, CHIPS, 1, 5, 2, 6, 3, 7):
        peer[i].start()

    def rcopy(src, dst, i, dev):
        return pltpu.make_async_remote_copy(src_ref=src, dst_ref=dst, send_sem=ssem.at[i], recv_sem=rsem.at[i],
                                            device_id={"ep": dev}, device_id_type=MESH)

    eg, ef, es = rcopy(eo.at[0], erg, PEERS, yn), rcopy(eo.at[1], erf, 9, yn), rcopy(eo.at[2], ers, 10, zn)
    back = rcopy(eo.at[3], ecr, 11, mir)
    gshare = rcopy(gw_ref, gsib, 12, sib)
    order = (1 - c, c)
    mg = [rcopy(mo.at[0, b], mrg.at[b], 13 + n, first) for n, b in enumerate(order)]
    ms = [rcopy(mo.at[2, b], mrs.at[b], 15 + n, second) for n, b in enumerate(order)]
    mf = rcopy(mo.at[1], mrf, 17, first)
    mfinal = rcopy(mo.at[3, 1 - c], mfin, 18, sib)

    def joined(own, got, i, base):
        local[base + i].wait()
        peer[base + i].wait_recv()
        own[i] = own[i] + got[i]

    joined(eo, ed, 0, 0)
    eg.start()
    joined(mo, md, 0, CHIPS)
    mg[0].start()
    joined(eo, ed, 1, 0)
    ef.start()
    mg[1].start()
    joined(eo, ed, 2, 0)
    joined(eo, ed, 3, 0)
    gshare.start()
    eg.wait_recv()
    eo[2] = eo[2] + erg[...]
    es.start()
    joined(mo, md, 1, CHIPS)
    mf.start()
    joined(mo, md, 2, CHIPS)
    mg[0].wait_recv()
    mo[2, 1 - c] = mo[2, 1 - c] + mrg[1 - c]
    ms[0].start()
    ef.wait_recv()
    es.wait_recv()
    eo[3] = eo[3] + erf[...] + ers[...]
    back.start()
    joined(mo, md, 3, CHIPS)
    out_ref[...] = z_ref[...]
    mg[1].wait_recv()
    mo[2, c] = mo[2, c] + mrg[c]
    ms[1].start()
    mf.wait_recv()
    mo[3] = mo[3] + mrf[...]
    gshare.wait_recv()
    back.wait_recv()
    for b, g in ((c, gw_ref), (1 - c, gsib)):
        for part in split3(g[...]):
            mo[3, b] += dot(part, ecr[b], 0, 0)
    ms[0].wait_recv()
    mo[3, 1 - c] = mo[3, 1 - c] + mrs[1 - c]
    mfinal.start()
    ms[1].wait_recv()
    out_ref[:, mine] += mo[3, c] + mrs[c]
    mfinal.wait_recv()
    out_ref[:, theirs] += mfin[...]
    y_ref[...] = out_ref[...].astype(y_ref.dtype)
    for cp in peer + mg + ms + [eg, ef, es, back, gshare, mf, mfinal]:
        cp.wait_send()


def solution(mesh):
    any_space = pl.BlockSpec(memory_space=pl.ANY)
    vmem = pl.BlockSpec(memory_space=pltpu.VMEM)
    smem = pl.BlockSpec(memory_space=pltpu.SMEM)
    sds = jax.ShapeDtypeStruct

    def gather(x, at, se, rnd, wr, w1, w3, w2):
        d, ff = w1.shape
        return pl.pallas_call(
            gather_kernel,
            out_shape=(sds((PEERS, LANES, d), BF16), sds((PEERS, EXT, d), BF16), sds((PEERS, 16, LANES), F32),
                       sds((PEERS, PEERS, LANES), F32), sds((PEERS, LANES), I32), sds((EXT, LANES), F32),
                       sds((LANES, d), F32), sds((1, 1), I32)),
            in_specs=[vmem, vmem, vmem, smem, vmem] + [any_space] * 3,
            out_specs=(any_space,) * CHIPS + (vmem,) * CHIPS,
            scratch_shapes=[
                pltpu.VMEM((PEERS, LANES, d), BF16), pltpu.VMEM((PEERS, EXT, d), BF16),
                pltpu.VMEM((PEERS, 16, LANES), F32), pltpu.VMEM((PEERS, PEERS, LANES), F32),
                pltpu.VMEM((EXT, d), BF16), pltpu.VMEM((PEERS, LANES), F32),
                pltpu.VMEM((EXT, d), BF16), pltpu.VMEM((PEERS, LANES), F32), pltpu.VMEM((16, LANES), F32),
                pltpu.VMEM((2, NUM_EXPERTS, LANES), F32), pltpu.VMEM((NUM_EXPERTS, LANES), F32),
                pltpu.VMEM((5, PEERS, LANES), F32), pltpu.VMEM((5, PEERS, LANES), F32),
                pltpu.VMEM((d, ff), BF16), pltpu.VMEM((d, ff), BF16), pltpu.VMEM((ff, d), BF16),
                pltpu.SemaphoreType.DMA((60,)), pltpu.SemaphoreType.DMA((60,)), pltpu.SemaphoreType.DMA((21,)),
            ],
            compiler_params=pltpu.CompilerParams(collective_id=0, has_side_effects=True),
            name="gather_rows",
        )(x, at, se, rnd, wr, w1, w3, w2)

    def experts(own, se, xm, xe, wm, we, w1, w3, w2):
        _, d, ff = w1.shape
        n_tok = PEERS * (LANES + EXT)
        return pl.pallas_call(
            expert_kernel,
            out_shape=(sds((PEERS * LANES, d), F32), sds((PEERS * EXT, d), BF16)),
            in_specs=[smem, smem, any_space, any_space, vmem, vmem] + [any_space] * 3,
            out_specs=(any_space, any_space),
            scratch_shapes=[
                pltpu.VMEM((n_tok, d), BF16), pltpu.VMEM((n_tok // LANES, NUM_EXPERTS, LANES), F32), pltpu.VMEM((n_tok // LANES, NUM_EXPERTS, LANES), F32),
                pltpu.VMEM((n_tok, d), F32), pltpu.VMEM((PEERS * EXT, d), BF16), pltpu.VMEM((MAXENT * UNIT, d), BF16),
                pltpu.VMEM((GROUP * TILE, d), BF16),
                pltpu.VMEM((NUM_EXPERTS, LANES), I32), pltpu.SMEM((NUM_EXPERTS, LANES), I32),
                pltpu.VMEM((NBUF, d, ff), BF16), pltpu.VMEM((NBUF, d, ff), BF16), pltpu.VMEM((NBUF, ff, d), BF16),
                pltpu.SMEM((32,), I32), pltpu.SMEM((32,), I32), pltpu.SMEM((NUM_EXPERTS,), I32),
                pltpu.SMEM((384,), I32), pltpu.SMEM((384,), I32), pltpu.SMEM((384,), I32),
                pltpu.SMEM((12 * TILES,), I32), pltpu.SMEM((12 * TILES,), I32), pltpu.SMEM((12 * TILES,), I32),
                pltpu.SMEM((16,), I32),
                pltpu.SemaphoreType.DMA((3, NBUF)), pltpu.SemaphoreType.DMA((3,)), pltpu.SemaphoreType.DMA((12,)),
            ],
            name="expert_rows",
        )(own, se, xm, xe, wm, we, w1, w3, w2)

    def scatter(pm, pe, z, gw, last):
        d = z.shape[1]
        half = d // 2
        big, small = (2, LANES, half), (2, EXT, half)
        return pl.pallas_call(
            scatter_kernel,
            out_shape=sds((LANES, d), BF16 if last else F32),
            in_specs=[any_space, any_space, vmem, vmem],
            out_specs=vmem,
            scratch_shapes=[
                pltpu.VMEM((LANES, d), F32),
                pltpu.VMEM((CHIPS,) + big, F32), pltpu.VMEM((CHIPS,) + big, F32),
                pltpu.VMEM(big, F32), pltpu.VMEM(big, F32), pltpu.VMEM(big, F32), pltpu.VMEM((LANES, half), F32),
                pltpu.VMEM((CHIPS,) + small, BF16), pltpu.VMEM((CHIPS,) + small, BF16),
                pltpu.VMEM(small, BF16), pltpu.VMEM(small, BF16), pltpu.VMEM(small, BF16), pltpu.VMEM((EXT, LANES), F32),
                pltpu.VMEM(small, BF16),
                pltpu.SemaphoreType.DMA((20,)), pltpu.SemaphoreType.DMA((20,)), pltpu.SemaphoreType.DMA((PEERS,)),
            ],
            compiler_params=pltpu.CompilerParams(collective_id=1 if last else 2, has_side_effects=True),
            name="scatter_sums" if last else "scatter_more",
        )(pm, pe, z, gw)

    def device_step(x, slot_expert, w1, w3, w2, assign, wr, w1s, w3s, w2s):
        d = x.shape[1]
        rows_of = lambda a: a.reshape(-1, d)

        def gathered(r):
            return gather(x, assign.T, slot_expert, r.reshape(1), wr.T, w1s, w3s, w2s)

        def summed(parts):
            xm, xe, wm, we, own = parts
            pm, pe = experts(own, slot_expert, rows_of(xm), rows_of(xe), wm, we, w1, w3, w2)
            return pm.reshape(PEERS, LANES, d), pe.reshape(PEERS, EXT, d)

        def again(carry):
            r, n, z = carry
            *parts, gw, _, _ = gathered(r)
            return r + 1, n, scatter(*summed(parts), z, gw, False)

        *parts, gw, z, nr = gathered(jnp.int32(0))
        z = lax.while_loop(lambda s: s[0] < s[1], again, (jnp.int32(1), nr.reshape(()), z))[2]
        return scatter(*summed(parts), z, gw, True)

    tok = P(("dp", "ep"), None)
    slot = P("ep", None, None)
    return jax.shard_map(device_step, mesh=mesh,
                         in_specs=(tok, P(), slot, slot, slot, tok, P(), P(), P(), P()),
                         out_specs=tok, check_vma=False)
```

```python
import functools

import jax
import jax.numpy as jnp
from jax import lax
from jax.experimental import pallas as pl
from jax.experimental.pallas import tpu as pltpu
from jax.sharding import PartitionSpec as P

ROUTE_SCALE = 2.5
LANES, PEERS, CHIPS = 128, 8, 4
ZERO, ONE = 0.0, 1.0
MESH = pl.DeviceIdType.MESH
NUM_EXPERTS = 64
EXT = 64
UNIT = LANES
PIECES = 2
NBUF = 6
MAXENT = 14
GROUP = 16
FEW = 4
TILES = 160
TILE_BITS = CHIPS
TILE = 1 << TILE_BITS
TAKE = 2
F32, BF16, I32 = jnp.float32, jnp.bfloat16, jnp.int32


def dims():
    me = lax.axis_index("ep")
    c, y, z, h = me % 2, (me // 2) % 2, (me // CHIPS) % 2, me // PEERS
    sib = me + 1 - 2 * c
    yn = me + 2 - CHIPS * y
    zn = me + CHIPS - PEERS * z
    mir = me + PEERS - 16 * h
    first = yn + c * (zn - yn)
    second = zn + c * (yn - zn)
    diag = yn + zn - me
    return me, c, h, sib, yn, zn, mir, first, second, diag


def barrier(peers):
    sem = pltpu.get_barrier_semaphore()
    for peer in peers:
        pl.semaphore_signal(sem, inc=1, device_id=peer, device_id_type=MESH)
    pl.semaphore_wait(sem, len(peers))


def dot(a, b, ca=1, cb=0):
    return lax.dot_general(a, b, (((ca,), (cb,)), ((), ())), preferred_element_type=F32)


def split3(v):
    hi = v.astype(BF16)
    rest = v - hi.astype(F32)
    mid = rest.astype(BF16)
    lo = (rest - mid.astype(F32)).astype(BF16)
    return hi, mid, lo


def gather_kernel(x_ref, at_ref, se_ref, rnd_ref, wr_ref, w1_hbm, w3_hbm, w2_hbm,
                  xm_out, xe_out, wm_out, we_out, own_out, gw_out, z_out, nr_out,
                  xs, xes, wms, wes, xcr, ecr, xsnd, esnd, wsnd, cand_s, own_s, flag_s, frecv,
                  w1s, w3s, w2s, ssem, rsem, lsem):
    me, c, h, sib, yn, zn, mir, first, second, diag = dims()
    dp = lax.axis_index("dp")
    qm, qf, qs, qg = me % PEERS, first % PEERS, second % PEERS, diag % PEERS
    loads = [pltpu.make_async_copy(a, b, lsem.at[i]) for i, (a, b) in
             enumerate(((w1_hbm, w1s), (w3_hbm, w3s), (w2_hbm, w2s)))]
    for cp in loads:
        cp.start()
    barrier([{"ep": sib}, {"ep": yn}, {"ep": zn}, {"ep": mir}, {"dp": 1 - dp}])

    def rcopy(src, dst, i, dev):
        return pltpu.make_async_remote_copy(src_ref=src, dst_ref=dst, send_sem=ssem.at[i], recv_sem=rsem.at[i],
                                            device_id=dev, device_id_type=MESH)

    def spread(own, buf, base, one, two):
        ep = lambda d: {"ep": d}
        q1, q2 = one % PEERS, two % PEERS
        return [rcopy(own, buf.at[qm], base, ep(one)), rcopy(own, buf.at[qm], base + 1, ep(two)),
                rcopy(own, buf.at[qm], base + 2, ep(sib)), rcopy(buf.at[q1], buf.at[q1], base + 3, ep(two)),
                rcopy(buf.at[q1], buf.at[q1], base + CHIPS, ep(sib)), rcopy(buf.at[q2], buf.at[q2], base + 5, ep(sib)),
                rcopy(buf.at[qg], buf.at[qg], base + 6, ep(sib))]

    parts = [pl.ds(i * (x_ref.shape[0] // PIECES), x_ref.shape[0] // PIECES) for i in range(PIECES)]
    ax = [spread(x_ref.at[r], xs.at[:, r], 45 + 7 * i, first, second) for i, r in enumerate(parts)]
    for i in range(2):
        ax[0][i].start()

    n_tok = x_ref.shape[0]
    n_slots = se_ref.shape[0]
    rnd = jnp.full((1, 1), rnd_ref[0], I32).astype(F32)
    first_round = jnp.where(rnd == ZERO, ONE, ZERO)
    expert_of = se_ref[...].reshape(1, n_slots)
    eye = (lax.broadcasted_iota(I32, (NUM_EXPERTS, n_slots), 0) == expert_of).astype(F32)
    eye_bf = eye.astype(BF16)
    lane_slot = lax.broadcasted_iota(I32, (1, n_slots), 1)
    per_half = n_slots // 2
    here = jnp.where((lane_slot >= h * per_half) & (lane_slot < (h + 1) * per_half), ONE, ZERO)
    avail = jnp.where(jnp.sum(eye * here, axis=1, keepdims=True) > ZERO, ONE, ZERO)
    row_slot = lax.broadcasted_iota(I32, (n_slots, n_tok), 0)
    hot = jnp.concatenate([(row_slot == at_ref[k:k + 1, :]).astype(F32).astype(BF16) for k in range(6)], axis=1)
    picks_all = dot(eye_bf, hot)
    picks = [picks_all[:, k * n_tok:(k + 1) * n_tok] for k in range(6)]
    code = lax.broadcasted_iota(I32, (NUM_EXPERTS, n_tok), 0).astype(F32) + ONE
    ids = [jnp.sum(p * code, axis=0, keepdims=True) for p in picks]
    miss = [jnp.sum(p * (ONE - avail), axis=0, keepdims=True) for p in picks]
    none = jnp.zeros((2, n_tok), F32)
    id_all = jnp.concatenate(ids + [none], axis=0)
    miss_all = jnp.concatenate(miss + [none], axis=0)

    upper = (lax.broadcasted_iota(I32, (n_tok, n_tok), 0) < lax.broadcasted_iota(I32, (n_tok, n_tok), 1))
    before = dot(miss_all.astype(BF16), upper.astype(F32).astype(BF16))
    offset = -EXT * rnd
    count = jnp.zeros((1, 1), F32)
    row_ext = lax.broadcasted_iota(I32, (EXT, n_tok), 0).astype(F32)
    sels = []
    for k in range(6):
        sels.append(jnp.where((row_ext == before[k:k + 1, :] + offset) & (miss[k] > ZERO), ONE, ZERO))
        mk = jnp.sum(miss[k], axis=1, keepdims=True)
        offset += mk
        count += mk
    take = functools.reduce(lambda a, b: a + b, sels)
    xsnd[...] = dot(take.astype(BF16), x_ref[...]).astype(BF16)
    piece = [pl.ds(i * (EXT // PIECES), EXT // PIECES) for i in range(PIECES)]
    cross = [rcopy(xsnd.at[r], xcr.at[r], 20 + i, {"ep": mir}) for i, r in enumerate(piece)]
    cross.append(rcopy(esnd, ecr, 19, {"ep": mir}))
    for cp in cross[:-1]:
        cp.start()
    codes = jnp.zeros((PEERS, EXT), F32)
    for k in range(6):
        codes += dot(jnp.broadcast_to(ids[k], (PEERS, n_tok)).astype(BF16), sels[k].astype(BF16), 1, 1)
    esnd[...] = jnp.concatenate([codes, jnp.zeros((PEERS, LANES - EXT), F32)], axis=1)
    cross[-1].start()
    for a in ax[1:]:
        for i in range(2):
            a[i].start()
    for a in ax:
        a[2].start()

    gate = jax.nn.sigmoid(dot(wr_ref[...], x_ref[...], 1, 1))
    picked = gate * functools.reduce(lambda a, b: a + b, picks)
    total = jnp.sum(picked, axis=0, keepdims=True)
    weight = ROUTE_SCALE * picked / jnp.maximum(total, 1e-30)
    wk = [jnp.sum(p * weight, axis=0, keepdims=True) for p in picks]
    w_all = jnp.concatenate(wk + [none], axis=0) * (ONE - miss_all) * first_round
    packed = jnp.concatenate([id_all, w_all], axis=0)
    wsnd[...] = packed
    wms[qm] = packed
    aw = spread(wsnd, wms, 7, first, second)
    for i in range(3):
        aw[i].start()
    gw_out[...] = functools.reduce(lambda a, b: a + b, [sel * w for sel, w in zip(sels, wk)])
    flag_s[0] = jnp.broadcast_to(jnp.floor((count + (EXT - 1)) * (ONE / EXT)), (PEERS, LANES))
    steps = [rcopy(flag_s.at[i], frecv.at[i], 14 + i, d) for i, d in
             enumerate(({"dp": 1 - dp}, {"ep": sib}, {"ep": mir}, {"ep": zn}, {"ep": yn}))]
    steps[0].start()

    def vote(i):
        steps[i].wait()
        flag_s[i + 1] = jnp.maximum(flag_s[i], frecv[i])
        steps[i + 1].start()

    outs = []

    def put_out(src, dst, i):
        outs.append(pltpu.make_async_copy(src, dst, lsem.at[i]))
        outs[-1].start()

    put_out(x_ref, xm_out.at[qm], 3)

    slot_row = lax.broadcasted_iota(I32, (n_slots, LANES), 0)
    lane_dev = lax.broadcasted_iota(I32, (n_slots, LANES), 1)
    lo = (lane_dev + PEERS * h) * (n_slots // 16)
    block = ((slot_row >= lo) & (slot_row < lo + n_slots // 16) & (lane_dev < PEERS)).astype(F32).astype(BF16)
    cand = jnp.where(dot(eye_bf, block) > ZERO, ONE, ZERO)
    several = jnp.where(jnp.sum(cand, axis=1, keepdims=True) > ONE, ONE, ZERO)
    lane = lax.broadcasted_iota(I32, (1, LANES), 1).astype(F32)
    block_key = jnp.where(cand > ZERO, jnp.broadcast_to(lane, cand.shape), 1e9)
    cand_s[0] = block_key
    there = jnp.where(jnp.sum(eye * (ONE - here), axis=1, keepdims=True) > ZERO, 2.0, 5.0)
    cand_s[1] = jnp.broadcast_to(several * there, cand.shape)
    load0 = jnp.sum(cand * (ONE - several) * there, axis=0, keepdims=True)

    def pick(e, load):
        key = cand_s[0, pl.ds(e, 1), :] + load * 256.0
        best = jnp.min(key, axis=1, keepdims=True)
        sel = jnp.where((key == best) & (key < 1e8), ONE, ZERO)
        own_s[pl.ds(e, 1), :] = sel
        return load + sel * cand_s[1, pl.ds(e, 1), :]

    load1 = lax.fori_loop(0, NUM_EXPERTS // 2, pick, load0)
    vote(0)

    for a in ax + [aw]:
        a[0].wait_recv()
        a[3].start()
        a[CHIPS].start()
    for a in ax + [aw]:
        a[1].wait_recv()
        a[5].start()
    put_out(xs.at[qf], xm_out.at[qf], CHIPS)
    put_out(xs.at[qs], xm_out.at[qs], 5)
    vote(1)
    lax.fori_loop(NUM_EXPERTS // 2, NUM_EXPERTS, pick, load1)
    mine = jnp.where(lax.broadcasted_iota(I32, (PEERS, LANES), 1) == qm, ONE, ZERO)
    own = dot(mine.astype(BF16), own_s[...].astype(BF16), 1, 1)
    own_out[...] = jnp.concatenate([own, jnp.zeros((PEERS, LANES - NUM_EXPERTS), F32)], axis=1).astype(I32)
    vote(2)

    ew = spread(ecr, wes, 24, zn, yn)
    ex = [spread(xcr.at[r], xes.at[:, r], 31 + 7 * i, zn, yn) for i, r in enumerate(piece)]
    for i, a in enumerate(ex):
        cross[i].wait_recv()
        for n in range(3):
            a[n].start()
    cross[-1].wait_recv()
    wes[qm] = ecr[...]
    for n in range(3):
        ew[n].start()
    put_out(xcr, xe_out.at[qm], 6)
    vote(3)

    for cp in loads:
        cp.wait()
    hg = dot(x_ref[...], w1s[...])
    hu = dot(x_ref[...], w3s[...])
    act = (jax.nn.silu(hg) * hu).astype(BF16)
    z_out[...] = dot(act, w2s[...]) * first_round

    for a in ex + [ew]:
        a[0].wait_recv()
        a[3].start()
        a[CHIPS].start()
    for a in ex + [ew]:
        a[1].wait_recv()
        a[5].start()
    put_out(xes.at[zn % PEERS], xe_out.at[zn % PEERS], 7)
    put_out(xes.at[yn % PEERS], xe_out.at[yn % PEERS], PEERS)
    for a in ax + [aw]:
        a[3].wait_recv()
        a[6].start()
    put_out(xs.at[qg], xm_out.at[qg], 9)
    for n, i in enumerate((2, CHIPS, 5, 6)):
        for a in ax + [aw]:
            a[i].wait_recv()
        q = (sib % PEERS, qs + 1 - 2 * c, qf + 1 - 2 * c, qg + 1 - 2 * c)[n]
        put_out(xs.at[q], xm_out.at[q], 10 + n)
    steps[CHIPS].wait()
    nr_out[...] = jnp.maximum(flag_s[CHIPS], frecv[CHIPS])[0:1, 0:1].astype(I32)
    for a in ex + [ew]:
        a[3].wait_recv()
        a[6].start()
    put_out(xes.at[qg], xe_out.at[qg], 14)
    for n, i in enumerate((2, CHIPS, 5, 6)):
        for a in ex + [ew]:
            a[i].wait_recv()
        q = (sib % PEERS, zn % PEERS + 1 - 2 * c, yn % PEERS + 1 - 2 * c, qg + 1 - 2 * c)[n]
        put_out(xes.at[q], xe_out.at[q], 15 + n)
    put_out(wms, wm_out, 19)
    put_out(wes, we_out, 20)
    for a in [aw, ew, cross] + ax + ex:
        for cp in a:
            cp.wait_send()
    for cp in outs:
        cp.wait()


def expert_kernel(own_ref, se_ref, xm_hbm, xe_hbm, wm_ref, we_ref, w1_hbm, w3_hbm, w2_hbm, pm_out, pe_out,
                  xv, wrow, rank, pv, pev, obuf, kb, startv, starts, b1, b3, b2, slots, experts, seen, ent_e, ent_u, ent_i,
                  tile_e, tile_row, tile_rank, n_tiles, wsem, xsem, osem):
    me = lax.axis_index("ep")
    n_local = w1_hbm.shape[0]
    n_main, n_ext = PEERS * LANES, PEERS * EXT
    n_tok = n_main + n_ext
    n_blk = n_tok // LANES
    xl = [pltpu.make_async_copy(xm_hbm, xv.at[pl.ds(0, n_main)], xsem.at[0]),
          pltpu.make_async_copy(xe_hbm, xv.at[pl.ds(n_main, n_ext)], xsem.at[1])]
    for cp in xl:
        cp.start()

    def clear(e, carry):
        seen[e] = 0
        return carry

    lax.fori_loop(0, NUM_EXPERTS, clear, 0)

    def listing(s, n):
        e = se_ref[me * n_local + s]
        use = (own_ref[0, e] == 1) & (seen[e] == 0)

        @pl.when(use)
        def _():
            slots[n] = s
            experts[n] = e
            seen[e] = 1
        return jnp.where(use, n + 1, n)

    n_act = lax.fori_loop(0, n_local, listing, 0)

    def fetch(i):
        s, b = slots[i], lax.rem(i, NBUF)
        return [pltpu.make_async_copy(w1_hbm.at[s], b1.at[b], wsem.at[0, b]),
                pltpu.make_async_copy(w3_hbm.at[s], b3.at[b], wsem.at[1, b]),
                pltpu.make_async_copy(w2_hbm.at[s], b2.at[b], wsem.at[2, b])]

    def start(i):
        @pl.when(i < n_act)
        def _():
            for cp in fetch(i):
                cp.start()

    for i in range(NBUF):
        start(i)

    upper = (lax.broadcasted_iota(I32, (LANES, LANES), 0) < lax.broadcasted_iota(I32, (LANES, LANES), 1))
    upper = upper.astype(F32).astype(BF16)
    lane = lax.broadcasted_iota(I32, (NUM_EXPERTS, LANES), 1)
    code = lax.broadcasted_iota(I32, (NUM_EXPERTS, LANES), 0).astype(F32) + ONE
    run = jnp.zeros((NUM_EXPERTS, 1), F32)
    table = jnp.zeros((NUM_EXPERTS, LANES), F32)
    for j in range(n_blk):
        if j < PEERS:
            blk = wm_ref[j]
            w = jnp.zeros((NUM_EXPERTS, LANES), F32)
            for k in range(6):
                w += jnp.where(code == blk[k:k + 1, :], blk[PEERS + k:9 + k, :], ZERO)
        else:
            ids = jnp.concatenate([we_ref[2 * (j - PEERS)][:1, :EXT], we_ref[2 * (j - PEERS) + 1][:1, :EXT]], axis=1)
            w = jnp.where(code == ids, ONE, ZERO)
        mask = jnp.where(w != ZERO, ONE, ZERO)
        pos = dot(mask.astype(BF16), upper) + run
        run += jnp.sum(mask, axis=1, keepdims=True)
        table += jnp.where(lane == j + 1, run, ZERO)
        rank[j] = jnp.where(mask > ZERO, pos, -ONE)
        wrow[j] = w
    startv[...] = table.astype(I32)
    tc = pltpu.make_async_copy(startv, starts, xsem.at[2])
    tc.start()
    tc.wait()

    def list_units(i, n):
        e = experts[i]
        units = (starts[e, n_blk] + UNIT - 1) >> 7

        def put(u, n):
            ent_e[n] = e
            ent_u[n] = u
            ent_i[n] = i
            return n + 1
        return lax.fori_loop(0, units, put, n)

    n_all = lax.fori_loop(0, n_act, list_units, 0)
    for cp in xl:
        cp.wait()

    def out_copies(j):
        if j < PEERS:
            return pltpu.make_async_copy(pv.at[pl.ds(j * LANES, LANES)], pm_out.at[pl.ds(j * LANES, LANES)], osem.at[j])
        return pltpu.make_async_copy(pev.at[pl.ds((j - PEERS) * LANES, LANES)], pe_out.at[pl.ds((j - PEERS) * LANES, LANES)], osem.at[j])

    def finish(j):
        if j >= PEERS:
            pev[(j - PEERS) * LANES:(j - 7) * LANES, :] = pv[j * LANES:(j + 1) * LANES, :].astype(BF16)
        out_copies(j).start()

    def flush(first, n_ent, last):
        for j in range(n_blk):
            n_tiles[j] = 0

        def list_tiles(g, carry):
            e, u = ent_e[first + g], ent_u[first + g] * UNIT
            def span(blocks, hi):
                for j in blocks:
                    lo, hi = hi, jnp.clip(starts[e, j + 1] - u, 0, UNIT)
                    k0 = lo >> TILE_BITS
                    k1 = jnp.where(hi > lo, ((hi - 1) >> TILE_BITS) + 1, k0)
                    t = n_tiles[j]

                    def put(k, t, j=j):
                        tile_e[j * TILES + t] = e
                        tile_row[j * TILES + t] = g * UNIT + k * TILE
                        tile_rank[j * TILES + t] = u + k * TILE

                    put(k0, t)
                    put(k0 + 1, t + 1)
                    n_tiles[j] = t + k1 - k0

                    @pl.when(k1 > k0 + 2)
                    def _():
                        lax.fori_loop(2, k1 - k0, lambda k, _: put(k0 + k, t + k), None)

            span(range(PEERS), jnp.clip(-u, 0, UNIT))

            @pl.when(starts[e, n_blk] > starts[e, PEERS])
            def _():
                span(range(PEERS, n_blk), jnp.clip(starts[e, PEERS] - u, 0, UNIT))
            return carry

        lax.fori_loop(0, n_ent, list_tiles, 0)
        for j in range(n_blk):
            n_tile = n_tiles[j]

            joint = GROUP if j < PEERS else FEW

            def one_pass(p, carry, j=j, n_tile=n_tile, joint=joint):
                parts = []
                for g in range(joint):
                    t = p * joint + g
                    live = t < n_tile
                    e = jnp.where(live, tile_e[j * TILES + t], 0)
                    at = jnp.where(live, tile_row[j * TILES + t], 0)
                    base = jnp.where(live, tile_rank[j * TILES + t], -1000)
                    kb[g * TILE:(g + 1) * TILE, :] = obuf[pl.ds(pl.multiple_of(at, TILE), TILE), :]
                    rows = lax.broadcasted_iota(I32, (TILE, LANES), 0) + base
                    hit = rows.astype(F32) == rank[j, pl.ds(e, 1), :]
                    parts.append(jnp.where(hit, wrow[j, pl.ds(e, 1), :], ZERO))
                st = jnp.transpose(jnp.concatenate(parts, axis=0))
                res = dot(jnp.concatenate(split3(st), axis=0), kb[:joint * TILE, :])
                res = res[:LANES] + res[LANES:256] + res[256:]
                fresh = (first == 0) & (p == 0)

                @pl.when(fresh)
                def _():
                    pv[j * LANES:(j + 1) * LANES, :] = res

                @pl.when(jnp.logical_not(fresh))
                def _():
                    pv[j * LANES:(j + 1) * LANES, :] += res
                return carry

            @pl.when((first == 0) & (n_tile == 0))
            def _():
                pv[j * LANES:(j + 1) * LANES, :] = jnp.zeros((LANES, pv.shape[1]), F32)
            lax.fori_loop(0, (n_tile + joint - 1) // joint, one_pass, 0)

            @pl.when(last)
            def _():
                finish(j)

    def wait_for(k, carry):
        for cp in fetch(k):
            cp.wait()
        return carry

    def batch(bt, nxt):
        first = bt * MAXENT
        n_ent = jnp.minimum(n_all - first, MAXENT)

        def collect(q, carry):
            es = [jnp.minimum(q * TAKE + g, n_ent - 1) + first for g in range(TAKE)]
            ext = functools.reduce(jnp.logical_or, [starts[ent_e[n], n_blk] > starts[ent_e[n], PEERS] for n in es])

            def take(width):
                sel = []
                for n in es:
                    rows = (lax.broadcasted_iota(I32, (UNIT, LANES), 0) + ent_u[n] * UNIT).astype(F32)
                    e = ent_e[n]
                    sel.append(jnp.concatenate([jnp.where(rows == rank[j, pl.ds(e, 1), :], ONE, ZERO).astype(BF16)
                                                for j in range(width // LANES)], axis=1))
                got = dot(jnp.concatenate(sel, axis=0), xv[:width, :])
                obuf[pl.ds(pl.multiple_of(q * TAKE * UNIT, UNIT), TAKE * UNIT), :] = got.astype(BF16)

            @pl.when(ext)
            def _():
                take(n_tok)

            @pl.when(jnp.logical_not(ext))
            def _():
                take(n_main)
            return carry

        lax.fori_loop(0, (n_ent + TAKE - 1) // TAKE, collect, 0)

        def run_ffn(k, nxt):
            i = ent_i[first + k]

            def settle(k, carry):
                wait_for(k, carry)

                @pl.when(k < i)
                def _():
                    start(k + NBUF)
                return carry
            lax.fori_loop(nxt, i + 1, settle, 0)
            b = lax.rem(i, NBUF)
            two = (k + 1 < n_ent) & (ent_i[first + k + 1] == i)

            def ffn(n):
                rows = pl.ds(pl.multiple_of(k * UNIT, UNIT), n)
                xg = obuf[rows, :]
                act = (jax.nn.silu(dot(xg, b1[b])) * dot(xg, b3[b])).astype(BF16)
                obuf[rows, :] = dot(act, b2[b]).astype(BF16)

            @pl.when(two)
            def _():
                ffn(2 * UNIT)

            @pl.when(jnp.logical_not(two))
            def _():
                ffn(UNIT)
            end = k + jnp.where(two, 2, 1)

            @pl.when((first + end == n_all) | (ent_i[first + end] != i))
            def _():
                start(i + NBUF)
            return end, jnp.maximum(nxt, i + 1)

        nxt = lax.while_loop(lambda s: s[0] < n_ent, lambda s: run_ffn(*s), (0, nxt))[1]
        flush(first, n_ent, first + n_ent == n_all)
        return nxt

    nxt = lax.fori_loop(0, (n_all + MAXENT - 1) // MAXENT, batch, 0)

    def drain(k, carry):
        wait_for(k, carry)
        start(k + NBUF)
        return carry

    lax.fori_loop(nxt, n_act, drain, 0)

    @pl.when(n_all == 0)
    def _():
        pv[...] = jnp.zeros_like(pv)
        for j in range(n_blk):
            finish(j)
    for j in range(n_blk):
        out_copies(j).wait()


def scatter_kernel(pm_hbm, pe_hbm, z_ref, gw_ref, y_ref,
                   out_ref, mo, md, mrg, mrf, mrs, mfin, eo, ed, erg, erf, ers, gsib, ecr, ssem, rsem, lsem):
    me, c, h, sib, yn, zn, mir, first, second, diag = dims()
    cols = mo.shape[-1]
    mine = pl.ds(pl.multiple_of(c * cols, LANES), cols)
    theirs = pl.ds(pl.multiple_of((1 - c) * cols, LANES), cols)
    local, peer = [], []
    for base, (src, own, got, chips, swap) in ((0, (pe_hbm, eo, ed, (diag, yn, zn, me), (0, 1, 2, 3))),
                                               (CHIPS, (pm_hbm, mo, md, (diag, first, second, me), (0, 2, 1, 3)))):
        for i in range(CHIPS):
            rows = pl.ds(2 * ((chips[i] % PEERS) // 2), 2)
            sib_rows = pl.ds(2 * ((chips[swap[i]] % PEERS) // 2), 2)
            local.append(pltpu.make_async_copy(src.at[rows, :, mine], own.at[i], lsem.at[base + i]))
            peer.append(pltpu.make_async_remote_copy(
                src_ref=src.at[sib_rows, :, theirs], dst_ref=got.at[i], send_sem=ssem.at[base + i],
                recv_sem=rsem.at[base + i], device_id={"ep": sib}, device_id_type=MESH))
    for i in (0, CHIPS, 1, 5, 2, 6, 3, 7):
        local[i].start()
    barrier([{"ep": sib}, {"ep": yn}, {"ep": zn}, {"ep": mir}])
    for i in (0, CHIPS, 1, 5, 2, 6, 3, 7):
        peer[i].start()

    def rcopy(src, dst, i, dev):
        return pltpu.make_async_remote_copy(src_ref=src, dst_ref=dst, send_sem=ssem.at[i], recv_sem=rsem.at[i],
                                            device_id={"ep": dev}, device_id_type=MESH)

    eg, ef, es = rcopy(eo.at[0], erg, PEERS, yn), rcopy(eo.at[1], erf, 9, yn), rcopy(eo.at[2], ers, 10, zn)
    back = rcopy(eo.at[3], ecr, 11, mir)
    gshare = rcopy(gw_ref, gsib, 12, sib)
    order = (1 - c, c)
    mg = [rcopy(mo.at[0, b], mrg.at[b], 13 + n, first) for n, b in enumerate(order)]
    ms = [rcopy(mo.at[2, b], mrs.at[b], 15 + n, second) for n, b in enumerate(order)]
    mf = rcopy(mo.at[1], mrf, 17, first)
    mfinal = rcopy(mo.at[3, 1 - c], mfin, 18, sib)

    def joined(own, got, i, base):
        local[base + i].wait()
        peer[base + i].wait_recv()
        own[i] = own[i] + got[i]

    joined(eo, ed, 0, 0)
    eg.start()
    joined(mo, md, 0, CHIPS)
    mg[0].start()
    joined(eo, ed, 1, 0)
    ef.start()
    mg[1].start()
    joined(eo, ed, 2, 0)
    joined(eo, ed, 3, 0)
    gshare.start()
    eg.wait_recv()
    eo[2] = eo[2] + erg[...]
    es.start()
    joined(mo, md, 1, CHIPS)
    mf.start()
    joined(mo, md, 2, CHIPS)
    mg[0].wait_recv()
    mo[2, 1 - c] = mo[2, 1 - c] + mrg[1 - c]
    ms[0].start()
    ef.wait_recv()
    es.wait_recv()
    eo[3] = eo[3] + erf[...] + ers[...]
    back.start()
    joined(mo, md, 3, CHIPS)
    out_ref[...] = z_ref[...]
    mg[1].wait_recv()
    mo[2, c] = mo[2, c] + mrg[c]
    ms[1].start()
    mf.wait_recv()
    mo[3] = mo[3] + mrf[...]
    gshare.wait_recv()
    back.wait_recv()
    for b, g in ((c, gw_ref), (1 - c, gsib)):
        for part in split3(g[...]):
            mo[3, b] += dot(part, ecr[b], 0, 0)
    ms[0].wait_recv()
    mo[3, 1 - c] = mo[3, 1 - c] + mrs[1 - c]
    mfinal.start()
    ms[1].wait_recv()
    out_ref[:, mine] += mo[3, c] + mrs[c]
    mfinal.wait_recv()
    out_ref[:, theirs] += mfin[...]
    y_ref[...] = out_ref[...].astype(y_ref.dtype)
    for cp in peer + mg + ms + [eg, ef, es, back, gshare, mf, mfinal]:
        cp.wait_send()


def solution(mesh):
    any_space = pl.BlockSpec(memory_space=pl.ANY)
    vmem = pl.BlockSpec(memory_space=pltpu.VMEM)
    smem = pl.BlockSpec(memory_space=pltpu.SMEM)
    sds = jax.ShapeDtypeStruct

    def gather(x, at, se, rnd, wr, w1, w3, w2):
        d, ff = w1.shape
        return pl.pallas_call(
            gather_kernel,
            out_shape=(sds((PEERS, LANES, d), BF16), sds((PEERS, EXT, d), BF16), sds((PEERS, 16, LANES), F32),
                       sds((PEERS, PEERS, LANES), F32), sds((PEERS, LANES), I32), sds((EXT, LANES), F32),
                       sds((LANES, d), F32), sds((1, 1), I32)),
            in_specs=[vmem, vmem, vmem, smem, vmem] + [any_space] * 3,
            out_specs=(any_space,) * CHIPS + (vmem,) * CHIPS,
            scratch_shapes=[
                pltpu.VMEM((PEERS, LANES, d), BF16), pltpu.VMEM((PEERS, EXT, d), BF16),
                pltpu.VMEM((PEERS, 16, LANES), F32), pltpu.VMEM((PEERS, PEERS, LANES), F32),
                pltpu.VMEM((EXT, d), BF16), pltpu.VMEM((PEERS, LANES), F32),
                pltpu.VMEM((EXT, d), BF16), pltpu.VMEM((PEERS, LANES), F32), pltpu.VMEM((16, LANES), F32),
                pltpu.VMEM((2, NUM_EXPERTS, LANES), F32), pltpu.VMEM((NUM_EXPERTS, LANES), F32),
                pltpu.VMEM((5, PEERS, LANES), F32), pltpu.VMEM((5, PEERS, LANES), F32),
                pltpu.VMEM((d, ff), BF16), pltpu.VMEM((d, ff), BF16), pltpu.VMEM((ff, d), BF16),
                pltpu.SemaphoreType.DMA((60,)), pltpu.SemaphoreType.DMA((60,)), pltpu.SemaphoreType.DMA((21,)),
            ],
            compiler_params=pltpu.CompilerParams(collective_id=0, has_side_effects=True),
            name="gather_rows",
        )(x, at, se, rnd, wr, w1, w3, w2)

    def experts(own, se, xm, xe, wm, we, w1, w3, w2):
        _, d, ff = w1.shape
        n_tok = PEERS * (LANES + EXT)
        return pl.pallas_call(
            expert_kernel,
            out_shape=(sds((PEERS * LANES, d), F32), sds((PEERS * EXT, d), BF16)),
            in_specs=[smem, smem, any_space, any_space, vmem, vmem] + [any_space] * 3,
            out_specs=(any_space, any_space),
            scratch_shapes=[
                pltpu.VMEM((n_tok, d), BF16), pltpu.VMEM((n_tok // LANES, NUM_EXPERTS, LANES), F32), pltpu.VMEM((n_tok // LANES, NUM_EXPERTS, LANES), F32),
                pltpu.VMEM((n_tok, d), F32), pltpu.VMEM((PEERS * EXT, d), BF16), pltpu.VMEM((MAXENT * UNIT, d), BF16),
                pltpu.VMEM((GROUP * TILE, d), BF16),
                pltpu.VMEM((NUM_EXPERTS, LANES), I32), pltpu.SMEM((NUM_EXPERTS, LANES), I32),
                pltpu.VMEM((NBUF, d, ff), BF16), pltpu.VMEM((NBUF, d, ff), BF16), pltpu.VMEM((NBUF, ff, d), BF16),
                pltpu.SMEM((32,), I32), pltpu.SMEM((32,), I32), pltpu.SMEM((NUM_EXPERTS,), I32),
                pltpu.SMEM((384,), I32), pltpu.SMEM((384,), I32), pltpu.SMEM((384,), I32),
                pltpu.SMEM((12 * TILES,), I32), pltpu.SMEM((12 * TILES,), I32), pltpu.SMEM((12 * TILES,), I32),
                pltpu.SMEM((16,), I32),
                pltpu.SemaphoreType.DMA((3, NBUF)), pltpu.SemaphoreType.DMA((3,)), pltpu.SemaphoreType.DMA((12,)),
            ],
            name="expert_rows",
        )(own, se, xm, xe, wm, we, w1, w3, w2)

    def scatter(pm, pe, z, gw, last):
        d = z.shape[1]
        half = d // 2
        big, small = (2, LANES, half), (2, EXT, half)
        return pl.pallas_call(
            scatter_kernel,
            out_shape=sds((LANES, d), BF16 if last else F32),
            in_specs=[any_space, any_space, vmem, vmem],
            out_specs=vmem,
            scratch_shapes=[
                pltpu.VMEM((LANES, d), F32),
                pltpu.VMEM((CHIPS,) + big, F32), pltpu.VMEM((CHIPS,) + big, F32),
                pltpu.VMEM(big, F32), pltpu.VMEM(big, F32), pltpu.VMEM(big, F32), pltpu.VMEM((LANES, half), F32),
                pltpu.VMEM((CHIPS,) + small, BF16), pltpu.VMEM((CHIPS,) + small, BF16),
                pltpu.VMEM(small, BF16), pltpu.VMEM(small, BF16), pltpu.VMEM(small, BF16), pltpu.VMEM((EXT, LANES), F32),
                pltpu.VMEM(small, BF16),
                pltpu.SemaphoreType.DMA((20,)), pltpu.SemaphoreType.DMA((20,)), pltpu.SemaphoreType.DMA((PEERS,)),
            ],
            compiler_params=pltpu.CompilerParams(collective_id=1 if last else 2, has_side_effects=True),
            name="scatter_sums" if last else "scatter_more",
        )(pm, pe, z, gw)

    def device_step(x, slot_expert, w1, w3, w2, assign, wr, w1s, w3s, w2s):
        d = x.shape[1]
        rows_of = lambda a: a.reshape(-1, d)

        def gathered(r):
            return gather(x, assign.T, slot_expert, r.reshape(1), wr.T, w1s, w3s, w2s)

        def summed(parts):
            xm, xe, wm, we, own = parts
            pm, pe = experts(own, slot_expert, rows_of(xm), rows_of(xe), wm, we, w1, w3, w2)
            return pm.reshape(PEERS, LANES, d), pe.reshape(PEERS, EXT, d)

        def again(carry):
            r, n, z = carry
            *parts, gw, _, _ = gathered(r)
            return r + 1, n, scatter(*summed(parts), z, gw, False)

        *parts, gw, z, nr = gathered(jnp.int32(0))
        z = lax.while_loop(lambda s: s[0] < s[1], again, (jnp.int32(1), nr.reshape(()), z))[2]
        return scatter(*summed(parts), z, gw, True)

    tok = P(("dp", "ep"), None)
    slot = P("ep", None, None)
    return jax.shard_map(device_step, mesh=mesh,
                         in_specs=(tok, P(), slot, slot, slot, tok, P(), P(), P(), P()),
                         out_specs=tok, check_vma=False)
```
